32 devices in a mesh: dp: 2 (over x), seq: 4 (over z), head: 4 (over y, core).
Axes of the slice: x: 2, y: 2, z: 4, core: 2. Of those that a mesh axis runs over, the one named last changes fastest.
Arguments:
- block_input: bfloat16 [4, 1024, 1536], P('dp', 'seq', 'head'), may hold values from -6 to 6
- norm_gain: bfloat16 [1536], P('head'), may hold values from 0.25 to 1.75
- w_gate: bfloat16 [1536, 3072], P(None, 'head'), may hold values from -0.15625 to 0.15625
- w_value: bfloat16 [1536, 3072], P(None, 'head'), may hold values from -0.15625 to 0.15625
- w_select: bfloat16 [1536, 256], P(None, 'head'), may hold values from -0.15625 to 0.15625
- w_step: bfloat16 [1536, 48], P(None, 'head'), may hold values from -0.15625 to 0.15625
- conv_value: float32 [4, 3072], P(None, 'head'), may hold values from -3 to 3
- bias_value: float32 [3072], P('head'), may hold values from -3 to 3
- conv_select: float32 [4, 256], P(None, 'head'), may hold values from -3 to 3
- bias_select: float32 [256], P('head'), may hold values from -3 to 3
- step_bias: float32 [48], P('head'), as said below
- decay_log: float32 [48], P('head'), may hold values from 0 to 1.4
- skip_gain: float32 [48], P('head'), may hold values from 0.5 to 1.5
- gate_gain: float32 [3072], P('head'), may hold values from 0.25 to 1.75
- w_out: bfloat16 [3072, 1536], P('head'), may hold values from -0.109375 to 0.109375
- out_cotangent: bfloat16 [4, 1024, 1536], P('dp', 'seq', 'head'), may hold values from -6 to 6
Outputs:
- block_output: bfloat16 [4, 1024, 1536], P('dp', 'seq', 'head')
- input_grad: float32 [4, 1024, 1536], P('dp', 'seq', 'head')
- grad_norm_gain: float32 [1536], P('head')
- grad_w_gate: float32 [1536, 3072], P(None, 'head')
- grad_w_value: float32 [1536, 3072], P(None, 'head')
- grad_w_select: float32 [1536, 256], P(None, 'head')
- grad_w_step: float32 [1536, 48], P(None, 'head')
- grad_conv_value: float32 [4, 3072], P(None, 'head')
- grad_bias_value: float32 [3072], P('head')
- grad_conv_select: float32 [4, 256], P(None, 'head')
- grad_bias_select: float32 [256], P('head')
- grad_step_bias: float32 [48], P('head')
- grad_decay_log: float32 [48], P('head')
- grad_skip_gain: float32 [48], P('head')
- grad_gate_gain: float32 [3072], P('head')
- grad_w_out: float32 [3072, 1536], P('head')
The draws below stay inside these ranges and needn't reach their ends.
Inputs may be any that keep to these rules, and one draw needn't show every extreme that they name: `step_bias`: every entry lies between -12 and -4.
All inputs are finite; a program needn't handle non-finite values.
Results may differ from the reference program's by a relative error of at most 0.012.
The reference program's roundings to bfloat16 on the way (of `normed` and `hidden`) count: a program that leaves them out, or rounds other values in their place, can miss the bound.
Values may be sent and summed in bfloat16 or wider, within the bound.
A program may use at most 128 MiB of HBM per device.

```python
import math
import jax
import jax.numpy as jnp
from jax import lax

D = 1536
HEADS = 48
HEAD_DIM = 64
STATE = 128
GROUP = 256
CONV = 4
LENGTH = 1024
INNER = 3072
SEQS = 4


def draw_step_bias(key, part):
    low_end = math.log(0.3 / LENGTH)
    high_end = math.log(1.0 / 24.0)
    log_rate = jax.random.uniform(key, (HEADS,), jnp.float32, low_end, high_end)
    step_target = jnp.exp(log_rate) / 3.3
    return jnp.log(jnp.expm1(step_target)).astype(jnp.float32)


def block_levels(key, extent, pieces, least, top_value):
    loudness, own = 1.0, jax.random.fold_in(key, 6)
    for dim, shards_of in pieces:
        steps = jnp.exp(jax.random.uniform(jax.random.fold_in(own, dim), (shards_of,), jnp.float32, least / len(pieces), top_value / len(pieces)))
        loudness = loudness * jnp.repeat(steps, extent[dim] // shards_of).reshape([-1 if axis == dim else 1 for axis in range(len(extent))])
    return loudness


def bell_draw(rng, extent, deviation, reach, pieces=(), kind=jnp.bfloat16):
    factor_of = block_levels(rng, extent, pieces, -0.22, 0.18) if pieces else 1.0
    values = jax.random.normal(rng, extent, jnp.float32) * deviation * factor_of
    return jnp.minimum(jnp.maximum(values, -reach), reach).astype(kind)


def setup_inputs(seed: int = 0) -> dict:
    seeds = jax.random.split(jax.random.key(seed), 17)
    return {
        "block_input": bell_draw(seeds[0], (SEQS, LENGTH, D), 1.0, 6.0, ((0, 2), (1, 4), (2, 4))),
        "norm_gain": jnp.clip(1.0 + 0.15 * jax.random.normal(seeds[1], (D,), jnp.float32), 0.25, 1.75).astype(jnp.bfloat16),
        "w_gate": bell_draw(seeds[2], (D, INNER), D ** -0.5, 0.15625, ((1, 4),)),
        "w_value": bell_draw(seeds[3], (D, INNER), D ** -0.5, 0.15625, ((1, 4),)),
        "w_select": bell_draw(seeds[4], (D, 2 * STATE), D ** -0.5, 0.15625, ((1, 4),)),
        "w_step": bell_draw(seeds[5], (D, HEADS), D ** -0.5, 0.15625, ((1, 4),)),
        "conv_value": bell_draw(seeds[6], (CONV, INNER), CONV ** -0.5, 3.0, ((1, 4),), jnp.float32),
        "bias_value": bell_draw(seeds[7], (INNER,), 0.5, 3.0, ((0, 4),), jnp.float32),
        "conv_select": bell_draw(seeds[8], (CONV, 2 * STATE), CONV ** -0.5, 3.0, ((1, 4),), jnp.float32),
        "bias_select": bell_draw(seeds[9], (2 * STATE,), 0.5, 3.0, ((0, 4),), jnp.float32),
        "step_bias": draw_step_bias(jax.random.fold_in(seeds[16], 71), 0),
        "decay_log": jnp.clip(1.4 * jax.random.uniform(seeds[11], (HEADS,), jnp.float32) ** block_levels(seeds[11], (HEADS,), ((0, 4),), -0.2, 0.2), 0.0, 1.4),
        "skip_gain": jnp.clip(0.5 + 1.0 * jax.random.uniform(seeds[12], (HEADS,), jnp.float32) ** block_levels(seeds[12], (HEADS,), ((0, 4),), -0.2, 0.2), 0.5, 1.5),
        "gate_gain": jnp.clip(1.0 + 0.15 * jax.random.normal(seeds[13], (INNER,), jnp.float32), 0.25, 1.75),
        "w_out": bell_draw(seeds[14], (INNER, D), INNER ** -0.5, 0.109375, ((0, 4),)),
        "out_cotangent": bell_draw(seeds[15], (SEQS, LENGTH, D), 1.0, 6.0, ((0, 2), (1, 4), (2, 4))),
    }


EPSILON = 1e-05
HIGHEST = lax.Precision.HIGHEST

def rms_norm(values, scale_vec):
    return values * lax.rsqrt(lax.optimization_barrier(jnp.mean(values * values, axis=-1, keepdims=True)) + EPSILON) * scale_vec

def causal_filter(pre_conv, weight, offset):
    length_now = pre_conv.shape[0]
    padded = jnp.concatenate([jnp.zeros((CONV - 1, pre_conv.shape[1]), pre_conv.dtype), pre_conv], axis=0)
    filtered = offset + weight[0] * padded[0:length_now]
    for lag_index in range(1, CONV):
        filtered = filtered + weight[lag_index] * padded[lag_index:lag_index + length_now]
    return jax.nn.silu(filtered)

def gated_norm(mixed_out, gate_in, scale_vec):
    gated_values = mixed_out * jax.nn.silu(gate_in)
    return gated_values * lax.rsqrt(lax.optimization_barrier(jnp.mean(gated_values * gated_values, axis=-1, keepdims=True)) + EPSILON) * scale_vec

def state_space(values, step_raw, step_bias, decay_log, in_state, out_state):
    total_len = values.shape[0]
    block_count = total_len // GROUP
    step_size = jax.nn.softplus(step_raw + step_bias)
    decay_rate = -jnp.exp(decay_log)
    cumulative = jnp.cumsum((step_size * decay_rate).reshape(block_count, GROUP, HEADS), axis=1)
    value_blocks = values.reshape(block_count, GROUP, HEADS, HEAD_DIM)
    in_blocks = in_state.reshape(block_count, GROUP, STATE)
    out_blocks = out_state.reshape(block_count, GROUP, STATE)
    step_blocks = step_size.reshape(block_count, GROUP, HEADS)
    causal_mask = jnp.tril(jnp.ones((GROUP, GROUP), dtype=bool))[None, :, :, None]
    log_gap = cumulative[:, :, None, :] - cumulative[:, None, :, :]
    decay_mat = jnp.exp(jnp.where(causal_mask, log_gap, -jnp.inf))
    scores = jnp.einsum('kqn,ktn->kqt', out_blocks, in_blocks, precision=HIGHEST)
    weighted = value_blocks * step_blocks[..., None]
    intra_part = jnp.einsum('kqth,kthp->kqhp', scores[..., None] * decay_mat, weighted, precision=HIGHEST)
    tail_decay = jnp.exp(cumulative[:, -1:, :] - cumulative)
    group_states = jnp.einsum('kthp,ktn->khpn', weighted * tail_decay[..., None], in_blocks, precision=HIGHEST)
    factors = jnp.exp(cumulative[:, -1, :])

    def advance(state_now, scanned):
        group_state, factor = scanned
        return (factor[:, None, None] * state_now + group_state, state_now)
    start_state = jnp.zeros((HEADS, HEAD_DIM, STATE), values.dtype)
    _, entering = lax.scan(advance, start_state, (group_states, factors))
    inter_part = jnp.einsum('kqn,khpn->kqhp', out_blocks, entering, precision=HIGHEST) * jnp.exp(cumulative)[..., None]
    return (intra_part + inter_part).reshape(total_len, HEADS, HEAD_DIM)

def reference(block_input, norm_gain, w_gate, w_value, w_select, w_step, conv_value, bias_value, conv_select, bias_select, step_bias, decay_log, skip_gain, gate_gain, w_out, out_cotangent):

    def one_sequence(running, inputs):
        source, cotangent = inputs
        total_len = source.shape[0]
        source_wide = source.astype(jnp.float32)
        normed_wide, norm_back = jax.vjp(rms_norm, source_wide, norm_gain.astype(jnp.float32))
        normed = normed_wide.astype(jnp.bfloat16)
        gate_pre = lax.optimization_barrier(jnp.dot(normed, w_gate, preferred_element_type=jnp.float32).astype(jnp.bfloat16))
        value_pre = lax.optimization_barrier(jnp.dot(normed, w_value, preferred_element_type=jnp.float32).astype(jnp.bfloat16))
        select_pre = lax.optimization_barrier(jnp.dot(normed, w_select, preferred_element_type=jnp.float32).astype(jnp.bfloat16))
        step_raw = jnp.dot(normed, w_step, preferred_element_type=jnp.float32)
        value_wide, value_back = jax.vjp(causal_filter, value_pre.astype(jnp.float32), conv_value, bias_value)
        select_wide, select_back = jax.vjp(causal_filter, select_pre.astype(jnp.float32), conv_select, bias_select)
        value_act = lax.optimization_barrier(value_wide.astype(jnp.bfloat16)).astype(jnp.float32)
        select_act = lax.optimization_barrier(select_wide.astype(jnp.bfloat16)).astype(jnp.float32)
        in_state = select_act[:, :STATE]
        out_state = select_act[:, STATE:]
        state_out, state_back = jax.vjp(state_space, value_act, step_raw, step_bias, decay_log, in_state, out_state)
        value_heads = value_act.reshape(total_len, HEADS, HEAD_DIM)
        mixed_out = (state_out + skip_gain[:, None] * value_heads).reshape(total_len, INNER)
        hidden_wide, gate_back = jax.vjp(gated_norm, mixed_out, gate_pre.astype(jnp.float32), gate_gain)
        hidden = hidden_wide.astype(jnp.bfloat16)
        block_output = (source_wide + jnp.dot(hidden, w_out, preferred_element_type=jnp.float32)).astype(jnp.bfloat16)
        grad_w_out = jnp.dot(hidden.T, cotangent, preferred_element_type=jnp.float32)
        d_hidden = jnp.dot(cotangent, w_out.T, preferred_element_type=jnp.float32)
        d_mixed, d_gate, grad_gate_gain = gate_back(d_hidden)
        d_heads = d_mixed.reshape(total_len, HEADS, HEAD_DIM)
        grad_skip_gain = lax.optimization_barrier(jnp.sum(d_heads * value_heads, axis=(0, 2)))
        d_value_ssd, d_step_raw, grad_step_bias, grad_decay_log, d_in_state, d_out_state = state_back(d_heads)
        d_value = (d_value_ssd.reshape(total_len, HEADS, HEAD_DIM) + skip_gain[:, None] * d_heads).reshape(total_len, INNER)
        d_value_pre, grad_conv_value, grad_bias_value = value_back(d_value)
        d_select_pre, grad_conv_select, grad_bias_select = select_back(jnp.concatenate([d_in_state, d_out_state], axis=-1))
        gate_low = d_gate.astype(jnp.bfloat16)
        value_low = d_value_pre.astype(jnp.bfloat16)
        select_low = d_select_pre.astype(jnp.bfloat16)
        step_low = d_step_raw.astype(jnp.bfloat16)
        grad_w_gate = jnp.dot(normed.T, gate_low, preferred_element_type=jnp.float32)
        grad_w_value = jnp.dot(normed.T, value_low, preferred_element_type=jnp.float32)
        grad_w_select = jnp.dot(normed.T, select_low, preferred_element_type=jnp.float32)
        grad_w_step = jnp.dot(normed.T, step_low, preferred_element_type=jnp.float32)
        d_normed = jnp.dot(gate_low, w_gate.T, preferred_element_type=jnp.float32)
        d_normed = d_normed + jnp.dot(value_low, w_value.T, preferred_element_type=jnp.float32)
        d_normed = d_normed + jnp.dot(select_low, w_select.T, preferred_element_type=jnp.float32)
        d_normed = d_normed + jnp.dot(step_low, w_step.T, preferred_element_type=jnp.float32)
        d_source, grad_norm_gain = norm_back(d_normed)
        input_grad = cotangent.astype(jnp.float32) + d_source
        fresh = (grad_norm_gain, grad_w_gate, grad_w_value, grad_w_select, grad_w_step, grad_conv_value, grad_bias_value, grad_conv_select, grad_bias_select, grad_step_bias, grad_decay_log, grad_skip_gain, grad_gate_gain, grad_w_out)
        summed = tuple((older + newer for older, newer in zip(running, fresh)))
        return (summed, (block_output, input_grad))
    shapes = (norm_gain, w_gate, w_value, w_select, w_step, conv_value, bias_value, conv_select, bias_select, step_bias, decay_log, skip_gain, gate_gain, w_out)
    start_sums = tuple((jnp.zeros(item.shape, jnp.float32) for item in shapes))
    final, stacked = lax.scan(one_sequence, start_sums, (block_input, out_cotangent))
    block_output, input_grad = stacked
    g_norm, g_gate, g_value, g_select, g_step, g_conv_value, g_bias_value, g_conv_select, g_bias_select, g_step_bias, g_decay, g_skip, g_gate_gain, g_out = final
    return (block_output, input_grad, g_norm, g_gate, g_value, g_select, g_step, g_conv_value, g_bias_value, g_conv_select, g_bias_select, g_step_bias, g_decay, g_skip, g_gate_gain, g_out)
```

```python
import functools
from types import SimpleNamespace

import jax
import jax.numpy as jnp
from jax import lax
from jax.experimental import pallas as pl
from jax.experimental.pallas import tpu as pltpu
from jax.sharding import PartitionSpec as P

EPSILON = 1e-05
LOW = jnp.bfloat16
WIDE = jnp.float32
MESH = pl.DeviceIdType.MESH
RIM = 8
NEVER = -1e30
HEAD, SEQ, DP = "head", "seq", "dp"


def product(left, right, left_dim=1, right_dim=0):
    return lax.dot_general(
        left,
        right,
        (((left_dim,), (right_dim,)), ((), ())),
        preferred_element_type=WIDE,
    )


def pieces_of(values, count):
    found = []
    for _ in range(count):
        low = values.astype(LOW)
        found.append(low)
        values = values - low.astype(WIDE)
    return found


def picked(left, table, left_dim=1, table_dim=0, count=3):
    parts = [product(part, table, left_dim, table_dim) for part in pieces_of(left, count)]
    return functools.reduce(jnp.add, parts[::-1])


def picked_by(table, right, table_dim=1, right_dim=0, count=3):
    parts = [product(table, part, table_dim, right_dim) for part in pieces_of(right, count)]
    return functools.reduce(jnp.add, parts[::-1])


def iota(shape, dim):
    return lax.broadcasted_iota(jnp.int32, shape, dim)


def sigmoid(values):
    return 1.0 / (1.0 + jnp.exp(-values))


def softplus(values):
    return jnp.maximum(values, 0.0) + jnp.log1p(jnp.exp(-jnp.abs(values)))


def block(start, size):
    return pl.ds(pl.multiple_of(start, size), size)


class Links:
    def __init__(self, send_sem, recv_sem):
        self.send_sem, self.recv_sem, self.count = send_sem, recv_sem, 0

    def reserve(self, number):
        first = self.count
        self.count += number
        return first

    def copy(self, source, target, where, slot=None):
        slot = self.reserve(1) if slot is None else slot
        return pltpu.make_async_remote_copy(
            src_ref=source,
            dst_ref=target,
            send_sem=self.send_sem.at[slot],
            recv_sem=self.recv_sem.at[slot],
            device_id=where,
            device_id_type=MESH,
        )


def mixer_kernel(size, *refs):
    r = SimpleNamespace(**dict(zip(size.names, refs, strict=True)))
    seqs, rows, heads, width = size.seqs, size.rows, size.heads, size.width
    inner, state, piece = size.inner, size.state, size.piece
    head_count, seq_count, dp_count = size.head_axis, size.seq_axis, size.dp_axis
    inner_total, model = inner * head_count, piece * head_count
    total_rows = seqs * rows
    half = state // 2
    links = Links(r.send_sem, r.recv_sem)
    h, s, d = lax.axis_index(HEAD), lax.axis_index(SEQ), lax.axis_index(DP)
    side, over, across = h ^ 1, h ^ 2, h ^ 3
    place = lax.rem(h, 2) * half
    spare = half - place

    loads = []
    weights = (
        (r.w_value, r.v_w_value),
        (r.w_gate, r.v_w_gate),
        (r.w_out, r.v_w_out),
    )
    for index, (source, target) in enumerate(weights):
        load = pltpu.make_async_copy(source, target, r.load_sem.at[index])
        load.start()
        loads.append(load)

    barrier = pltpu.get_barrier_semaphore()
    peers = [{HEAD: lax.rem(h + j, head_count)} for j in range(1, head_count)]
    peers += [{SEQ: lax.rem(s + j, seq_count)} for j in range(1, seq_count)]
    peers += [{DP: lax.rem(d + j, dp_count)} for j in range(1, dp_count)]
    for peer in peers:
        pl.semaphore_signal(barrier, inc=1, device_id=peer, device_id_type=MESH)
    pl.semaphore_wait(barrier, len(peers))

    def gather_start(own, held):
        near = links.copy(own, held.at[h], {HEAD: side})
        far = links.copy(own, held.at[h], {HEAD: over})
        far.start()
        near.start()
        return (near, far)

    def gather_pass(held, pair):
        pair[1].wait_recv()
        forward = links.copy(held.at[over], held.at[over], {HEAD: side})
        forward.start()
        return pair + (forward,)

    def gather_end(copies):
        copies[0].wait_recv()
        copies[2].wait_recv()
        for copy in copies:
            copy.wait_send()

    r.gain_all[h] = jnp.broadcast_to(r.vec[0:1, size.norm_at : size.norm_at + piece], (8, piece))
    gain_copies = gather_start(r.gain_all.at[h], r.gain_all)
    input_copies = gather_start(r.x, r.x_all)
    cot_copies = gather_start(r.cot, r.cot_all)

    own_x = pltpu.make_async_copy(r.x, r.x_all.at[h], r.load_sem.at[3])
    own_cot = pltpu.make_async_copy(r.cot, r.cot_all.at[h], r.load_sem.at[4])
    own_x.start()
    own_cot.start()

    odd = lax.rem(h, 2) == 1
    r.expand[...] = jnp.where(
        (iota((state, inner), 1) // width + spare) == iota((state, inner), 0), 1.0, 0.0
    ).astype(LOW)
    lower = iota((rows, rows), 0) >= iota((rows, rows), 1)
    r.tri[...] = jnp.where(lower, 1.0, 0.0).astype(LOW)
    shift = jnp.where(iota((half, state), 0) + place == iota((half, state), 1), 1.0, 0.0).astype(LOW)
    r.taps[0:4, :] = picked(r.conv_select[...], shift)
    few = jnp.broadcast_to(r.vec[0:1, size.select_at : size.select_at + half], (8, half))
    r.taps[4:5, :] = picked(few, shift)[0:1, :]
    for row, start in enumerate((size.bias_at, size.decay_at, size.skip_at)):
        low_lanes = jnp.broadcast_to(r.vec[0:1, start : start + state], (8, state))
        r.taps[5 + row : 6 + row, :] = jnp.where(odd, low_lanes, pltpu.roll(low_lanes, half, 1))[0:1, :]
    r.v_w_select[...] = jnp.zeros((state, model), LOW)
    r.v_w_select[pl.ds(pl.multiple_of(place, half), half), :] = r.w_select[...]
    padded = jnp.concatenate([r.w_step[...], jnp.zeros((16 - heads, model), LOW)], axis=0)
    r.v_w_select[pl.ds(pl.multiple_of(spare, half), 16), :] = padded

    @pl.when(s == 0)
    def _():
        r.value_ext[:, 0:RIM, :] = jnp.zeros((seqs, RIM, inner), WIDE)
        r.select_ext[:, 0:RIM, :] = jnp.zeros((seqs, RIM, state), WIDE)
        r.state_in[...] = jnp.zeros((seqs, inner, state), LOW)

    @pl.when(s == seq_count - 1)
    def _():
        r.slope_v[:, rows : rows + RIM, :] = jnp.zeros((seqs, RIM, inner), WIDE)
        r.slope_s[:, rows : rows + RIM, :] = jnp.zeros((seqs, RIM, state), WIDE)
        r.adj_in[...] = jnp.zeros((seqs, inner, state), LOW)

    gain_copies = gather_pass(r.gain_all, gain_copies)
    input_copies = gather_pass(r.x_all, input_copies)
    gather_end(gain_copies)
    gather_end(input_copies)
    own_x.wait()

    def norm_rows(i, _):
        at = block(i * 64, 64)
        total = jnp.zeros((64, 1), WIDE)
        for k in range(head_count):
            part = r.x_all[k, at, :].astype(WIDE)
            total = total + jnp.sum(part * part, axis=1, keepdims=True)
        inverse = lax.rsqrt(total / model + EPSILON)
        r.inverse[at, :] = jnp.broadcast_to(inverse, (64, state))
        for k in range(head_count):
            part = r.x_all[k, at, :].astype(WIDE)
            r.normed[at, k * piece : (k + 1) * piece] = (
                part * inverse * r.gain_all[k, 0:1, :]
            ).astype(LOW)
        return 0

    lax.fori_loop(0, total_rows // 64, norm_rows, 0)

    for q in range(seqs):
        at = pl.ds(q * rows, rows)
        both = product(r.normed[at, :], r.v_w_select[...], 1, 1)
        r.step_arg[q] = both + r.taps[5:6, :]
        r.select_ext[q, RIM : RIM + rows, :] = both.astype(LOW).astype(WIDE)
    loads[0].wait()

    def value_matmul(q, _):
        at = block(q * rows, rows)
        r.value_ext[q, RIM : RIM + rows, :] = (
            product(r.normed[at, :], r.v_w_value[...]).astype(LOW).astype(WIDE)
        )
        return 0

    lax.fori_loop(0, seqs, value_matmul, 0)
    rims = []
    for ext in (r.select_ext, r.value_ext):
        for q in range(seqs):
            rims.append(
                links.copy(
                    ext.at[q, rows : rows + RIM, :],
                    ext.at[q, 0:RIM, :],
                    {SEQ: lax.rem(s + 1, seq_count)},
                )
            )

    @pl.when(s < seq_count - 1)
    def _():
        for copy in rims:
            copy.start()

    cot_copies = gather_pass(r.cot_all, cot_copies)

    tri = r.tri
    for q in range(seqs):
        step = softplus(r.step_arg[q])
        r.step[q] = step
        rate = -jnp.exp(r.taps[6:7, :])
        fall = step * rate
        running = picked_by(tri[...], fall)
        r.running[q] = running
        r.running_t[q] = picked(fall, tri[...], 0, 1)

        def spread(g, _):
            pick = jnp.where(iota((state, state), 0) == spare + g, 1.0, 0.0).astype(LOW)
            r.running_x[q, :, block(g * state, state)] = picked(r.running[q], pick)
            return 0

        lax.fori_loop(0, heads, spread, 0)
        r.step_x[q] = picked(step, r.expand[...], count=2)
        last = running[rows - 1 : rows, :]
        r.scale_x[q] = picked(jnp.exp(last - running), r.expand[...], count=2)
        decay = jnp.broadcast_to(jnp.exp(r.running_t[q, :, rows - 1 : rows]), (state, state))
        r.decay_row[q] = picked_by(r.expand[...], decay, 0, 0, count=2)

    @pl.when(s > 0)
    def _():
        for copy in rims:
            copy.wait_recv()

    @pl.when(s < seq_count - 1)
    def _():
        for copy in rims:
            copy.wait_send()

    lane_row = iota((1, state), 1)
    mine = (lane_row >= place) & (lane_row < place + half)

    def convolve(ext, q, base, count, taps, bias):
        wide = ext[q, pl.ds(pl.multiple_of(base, 8), count + RIM), :]
        total = bias
        for k in range(4):
            total = total + taps[k : k + 1, :] * wide[RIM - 3 + k : RIM - 3 + k + count]
        return total

    value_bias, gate_gain = r.vec[0:1, 0:inner], r.vec[0:1, inner : 2 * inner]

    for q in range(seqs):
        conv = convolve(r.select_ext, q, 0, rows, r.taps, r.taps[4:5, :])
        act = jnp.where(mine, conv * sigmoid(conv), 0.0)
        r.select_own[q] = act.astype(LOW)
    pair = links.copy(r.select_own, r.select_side, {HEAD: side})
    pair.start()

    def value_conv(i, _):
        q, base = i // (rows // 64), lax.rem(i, rows // 64) * 64
        conv = convolve(r.value_ext, q, base, 64, r.conv_value, value_bias)
        act = (conv * sigmoid(conv)).astype(LOW)
        at = block(base, 64)
        r.act[q, at, :] = act
        r.weighted[q, at, :] = (act.astype(WIDE) * r.step_x[q, at, :]).astype(LOW)
        return 0

    lax.fori_loop(0, seqs * (rows // 64), value_conv, 0)
    pair.wait()
    r.select_pair[...] = r.select_own[...] + r.select_side[...]
    swap = links.copy(r.select_pair, r.select_over, {HEAD: over})
    swap.start()
    loads[1].wait()

    def gate_matmul(q, _):
        at = block(q * rows, rows)
        r.gate[at, :] = product(r.normed[at, :], r.v_w_gate[...]).astype(LOW)
        return 0

    lax.fori_loop(0, seqs, gate_matmul, 0)
    swap.wait()
    upper = h >= 2
    first, second = r.select_pair[...], r.select_over[...]
    r.b_all[...] = jnp.where(upper, second, first)
    r.c_all[...] = jnp.where(upper, first, second)

    for q in range(seqs):
        b = r.b_all[q]
        tailed = (r.weighted[q].astype(WIDE) * r.scale_x[q]).astype(LOW)
        r.weighted_tail[q] = tailed
        r.state_local[q] = product(tailed, b, 0, 0)
        r.gram[q] = product(r.c_all[q], b, 1, 1)
        r.scale_x[q] = picked(jnp.exp(r.running[q]), r.expand[...], count=2)

    chunk_rows = inner // 3

    chunk_total = 3 * seqs

    def hop_copy(held, sent, first, c, forward):
        at = pl.ds(pl.multiple_of(lax.rem(c, 3) * chunk_rows, 16), chunk_rows)
        to = lax.rem(s + (1 if forward else seq_count - 1), seq_count)
        return at, links.copy(sent.at[c // 3, at, :], held.at[c // 3, at, :], {SEQ: to}, first + c)

    def hop(held, local, sent, first, c, forward):
        q = c // 3
        at, copy = hop_copy(held, sent, first, c, forward)

        @pl.when((s > 0) if forward else (s < seq_count - 1))
        def _():
            copy.wait_recv()

        sent[q, at, :] = (
            local[q, at, :] + r.decay_row[q, at, :] * held[q, at, :].astype(WIDE)
        ).astype(LOW)

        @pl.when((s < seq_count - 1) if forward else (s > 0))
        def _():
            copy.start()

    half_lane = iota((rows, state), 1) < width

    def decay_of(q, g):
        column = r.running_x[q, :, block(g * state, state)]
        gap = jnp.concatenate([column] * (rows // state), axis=1) - r.running_t[q, pl.ds(spare + g, 1), :]
        return jnp.exp(jnp.where(lower, gap, NEVER))

    def forward_pair(i, _):
        q, j = i // (heads // 2), lax.rem(i, heads // 2)
        at = block(j * state, state)
        values = r.weighted[q, :, at]
        zero = jnp.zeros_like(values)
        total = jnp.zeros((rows, state), WIDE)
        for part in range(2):
            mixing = (r.gram[q] * decay_of(q, 2 * j + part)).astype(LOW)
            kept = jnp.where(half_lane if part == 0 else ~half_lane, values, zero)
            total = total + product(mixing, kept)
        r.mixed[q, :, at] = total
        return 0

    pair_total = seqs * heads // 2
    forward_first = links.reserve(chunk_total)

    def forward_slot(i, _):
        @pl.when(i < pair_total)
        def _():
            forward_pair(i, 0)

        c = i - chunk_total * s

        @pl.when((c >= 0) & (c < chunk_total))
        def _():
            hop(r.state_in, r.state_local, r.state_out, forward_first, c, True)

        return 0

    lax.fori_loop(0, pair_total, forward_slot, 0)
    gather_end(cot_copies)
    own_cot.wait()
    loads[2].wait()

    def d_hidden_matmul(q, _):
        at = block(q * rows, rows)
        total = product(r.cot_all[0, at, :], r.v_w_out[:, 0:piece], 1, 1)
        for k in range(1, head_count):
            total = total + product(
                r.cot_all[k, at, :], r.v_w_out[:, k * piece : (k + 1) * piece], 1, 1
            )
        r.projected[q] = total
        return 0

    lax.fori_loop(0, seqs, d_hidden_matmul, 0)
    lax.fori_loop(pair_total, max(pair_total, chunk_total * seq_count), forward_slot, 0)

    r.skip_x[...] = picked(jnp.broadcast_to(r.taps[7:8, :], (8, state)), r.expand[...])
    for q in range(seqs):
        r.inter[q] = product(r.c_all[q], r.state_in[q], 1, 1) * r.scale_x[q]

    tile = 32
    lanes_tile = iota((tile, state), 1)

    def gate_rows(i, _):
        q, base = i // (rows // tile), lax.rem(i, rows // tile) * tile
        at, flat = block(base, tile), block(i * tile, tile)
        mixed = (
            r.mixed[q, at, :]
            + r.inter[q, at, :]
            + r.skip_x[0:1, :] * r.act[q, at, :].astype(WIDE)
        )
        r.mixed[q, at, :] = mixed
        gate = r.gate[flat, :].astype(WIDE)
        gated = mixed * (gate * sigmoid(gate))
        squares = jnp.sum(gated * gated, axis=1, keepdims=True)
        dots = jnp.sum(gated * r.projected[q, at, :] * gate_gain, axis=1, keepdims=True)
        r.sums[flat, :] = jnp.where(lanes_tile == 0, squares, jnp.where(lanes_tile == 1, dots, 0.0))
        return 0

    lax.fori_loop(0, total_rows // tile, gate_rows, 0)
    picks = jnp.where(iota((8, state), 0) == iota((8, state), 1), 1.0, 0.0).astype(LOW)

    def row_sums(own, held):
        own[...] = picked_by(picks, r.sums[...], 1, 1)
        copies = []
        for j in range(1, head_count):
            copy = links.copy(own, held.at[j - 1], {HEAD: h ^ j})
            copy.start()
            copies.append(copy)
        return copies

    def row_sums_end(own, held, copies):
        total = own[...]
        for j, copy in enumerate(copies):
            copy.wait_recv()
            total = total + held[j]
        r.sums[...] = picked(total, picks, 0, 0)
        for copy in copies:
            copy.wait_send()

    sum_copies = row_sums(r.sum_own, r.sum_held)

    @pl.when(s < seq_count - 1)
    def _():
        for c in range(chunk_total):
            hop_copy(r.state_in, r.state_out, forward_first, c, True)[1].wait_send()

    row_sums_end(r.sum_own, r.sum_held, sum_copies)

    small = r.small
    small[...] = jnp.zeros(small.shape, WIDE)

    def norm_back(i, carry):
        gain_total, skip_total = carry
        q, base = i // (rows // tile), lax.rem(i, rows // tile) * tile
        at, flat = block(base, tile), block(i * tile, tile)
        sums = r.sums[flat, :]
        scale = lax.rsqrt(sums[:, 0:1] / inner_total + EPSILON)
        mean = scale * scale * scale * (sums[:, 1:2] / inner_total)
        mixed = r.mixed[q, at, :]
        gate = r.gate[flat, :].astype(WIDE)
        logistic = sigmoid(gate)
        gate_act = gate * logistic
        gated = mixed * gate_act
        normal = gated * scale
        grad = r.projected[q, at, :]
        gain = gate_gain
        r.hidden[flat, :] = (normal * gain).astype(LOW)
        d_gated = scale * (grad * gain) - gated * mean
        d_mixed = d_gated * gate_act
        r.d_mixed_low[q, at, :] = d_mixed.astype(LOW)
        r.d_growth[q, at, :] = (d_mixed * r.scale_x[q, at, :]).astype(LOW)
        r.gate_low[flat, :] = (
            d_gated * mixed * (logistic * (1.0 + gate * (1.0 - logistic)))
        ).astype(LOW)
        gain_part = grad * normal
        skip_part = d_mixed * r.act[q, at, :].astype(WIDE)
        for k in range(tile // 8):
            gain_total = gain_total + gain_part[k * 8 : k * 8 + 8]
            skip_total = skip_total + skip_part[k * 8 : k * 8 + 8]
        return gain_total, skip_total

    blank = jnp.zeros((8, inner), WIDE)
    gain_total, skip_total = lax.fori_loop(0, total_rows // tile, norm_back, (blank, blank))
    small[5:6, 0:inner] = jnp.sum(gain_total, axis=0, keepdims=True)
    lanes = slice(inner + state, inner + 2 * state)
    skip_total = jnp.broadcast_to(jnp.sum(skip_total, axis=0, keepdims=True), (8, inner))
    small[2:3, lanes] = picked(skip_total, r.expand[...], 1, 1)[0:1, :]

    for q in range(seqs):
        r.state_local[q] = product(r.d_growth[q], r.c_all[q], 0, 0)

    ends = (s == 0) | (s == seq_count - 1)
    inside = (s > 0) & (s < seq_count - 1)

    def rows_of(me, p):
        return pl.ds(pl.multiple_of((me.chunk * dp_count + p) * me.depth, 16), me.depth)

    def stream_start(bufs, chunk):
        part, over, up, mid, out = bufs
        me = SimpleNamespace(part=part, out=out, chunk=chunk, depth=up.shape[1])
        me.over, me.up, me.mid = over.at[chunk], up.at[chunk], mid.at[chunk]
        own = part.at[rows_of(me, d), :]
        me.copies = []
        for j in range(1, dp_count):
            to = lax.rem(d + j, dp_count)
            copy = links.copy(part.at[rows_of(me, to), :], me.over.at[j - 1], {DP: to})
            copy.start()
            me.copies.append(copy)
        me.copy_up = links.copy(own, me.up, {SEQ: s ^ 1})
        me.copy_mid = links.copy(own, me.mid, {SEQ: seq_count - 1 - s})
        me.copy_down = links.copy(me.up, me.up, {SEQ: s ^ 1})
        target = out.at[rows_of(me, d), :]
        me.keep = pltpu.make_async_copy(me.up, target, r.keep_sem.at[len(keeps)])
        keeps.append(me)
        me.copies_out = [
            links.copy(me.up, target, {DP: lax.rem(d + j, dp_count)}) for j in range(1, dp_count)
        ]
        return me

    keeps = []

    def add_rows(me, target, terms):
        depth = me.depth
        step = next(t for t in (64, 48, 16) if depth % t == 0)

        def add(i, _):
            at = pl.ds(pl.multiple_of(i * step, 16), step)
            own = pl.ds(pl.multiple_of((me.chunk * dp_count + d) * depth + i * step, 16), step)
            total = me.part[own, :].astype(WIDE)
            for term in terms:
                total = total + term[at, :].astype(WIDE)
            if target is None:
                me.part[own, :] = total.astype(LOW)
            else:
                target[at, :] = total.astype(LOW)
            return 0

        lax.fori_loop(0, depth // step, add, 0)

    def stream_a(me):
        for copy in me.copies:
            copy.wait_recv()
        add_rows(me, None, [me.over.at[j] for j in range(dp_count - 1)])

        @pl.when(ends)
        def _():
            me.copy_up.start()

    def stream_b(me):
        @pl.when(inside)
        def _():
            me.copy_up.wait_recv()
            add_rows(me, None, [me.up])
            me.copy_mid.start()

    def stream_c(me):
        @pl.when(inside)
        def _():
            me.copy_mid.wait_recv()
            add_rows(me, me.up, [me.mid])
            me.copy_down.start()

        @pl.when(ends)
        def _():
            me.copy_down.wait_recv()

        me.keep.start()
        for copy in me.copies_out:
            copy.start()

    def stream_d(me):
        for copy in me.copies_out:
            copy.wait()
        for copy in me.copies:
            copy.wait_send()
        me.keep.wait()

        @pl.when(ends)
        def _():
            me.copy_up.wait_send()

        @pl.when(inside)
        def _():
            me.copy_mid.wait_send()
            me.copy_down.wait_send()

    def big_grad(part, left, right, lanes):
        for start in range(0, part.shape[0], lanes):
            columns = slice(start, start + lanes)
            part[columns, :] = product(left[:, columns], right, 0, 0).astype(LOW)

    bufs_gate = (r.part_gate, r.over_gate, r.up_gate, r.mid_gate, r.out_gate)
    bufs_out = (r.v_w_out, r.over_out, r.up_out, r.mid_out, r.out_out)
    bufs_value = (r.part_value, r.over_value, r.up_value, r.mid_value, r.out_value)
    bufs_select = (r.part_select, r.over_select, r.up_select, r.mid_select, r.out_select)
    big_grad(r.part_gate, r.normed, r.gate_low[...], piece)
    gate_streams = [stream_start(bufs_gate, c) for c in range(r.up_gate.shape[0])]

    def spread_parts(part, near):
        copies = [
            links.copy(part.at[side], near.at[0], {HEAD: side}),
            links.copy(part.at[across], near.at[1], {HEAD: side}),
        ]
        for copy in copies:
            copy.start()
        return copies

    def spread_over(part, near, sent, far, copies):
        for copy in copies:
            copy.wait_recv()

        def add(i, _):
            at = block(i * 64, 64)
            sent[at, :] = (
                part[over, at, :].astype(WIDE) + near[1, at, :].astype(WIDE)
            ).astype(LOW)
            return 0

        lax.fori_loop(0, total_rows // 64, add, 0)
        last = links.copy(sent, far, {HEAD: over})
        last.start()
        for copy in copies:
            copy.wait_send()
        return last

    for k in range(head_count):
        r.branch[k] = product(
            r.hidden[...], r.v_w_out[:, k * piece : (k + 1) * piece]
        ).astype(LOW)
    branch_copies = spread_parts(r.branch, r.branch_near)
    for k in range(head_count):
        columns = slice(k * piece, (k + 1) * piece)
        r.v_w_out[:, columns] = product(r.hidden[...], r.cot_all[k], 0, 0).astype(LOW)
    out_streams = [stream_start(bufs_out, c) for c in range(r.up_out.shape[0])]

    r.pair_weight[...] = jnp.zeros((seqs, rows, rows), WIDE)
    r.row_part[...] = jnp.zeros((seqs, rows, state), WIDE)
    r.col_part[...] = jnp.zeros((seqs, state, rows), WIDE)
    head_lane = iota((1, state), 1)

    upper_tri = iota((rows, rows), 0) <= iota((rows, rows), 1)

    def backward_pair(i, _):
        q, j = i // (heads // 2), lax.rem(i, heads // 2)
        at = block(j * state, state)
        grads, values = r.d_mixed_low[q, :, at], r.weighted[q, :, at]
        gram = r.gram[q]
        zero = jnp.zeros_like(grads)
        total = jnp.zeros((rows, state), WIDE)
        for part in range(2):
            g = 2 * j + part
            column = r.running_x[q, :, block(g * state, state)]
            gap = r.running_t[q, pl.ds(spare + g, 1), :] - jnp.concatenate(
                [column] * (rows // state), axis=1
            )
            decay = jnp.exp(jnp.where(upper_tri, gap, NEVER))
            kept = jnp.where(half_lane if part == 0 else ~half_lane, grads, zero)
            total = total + product((gram * decay).astype(LOW), kept)
            pairs = decay * product(values, kept, 1, 1)
            r.pair_weight[q] += pairs
            flows = pairs * gram
            r.row_part[q] += jnp.where(
                head_lane == spare + g, jnp.sum(flows, axis=1, keepdims=True), 0.0
            )
            r.col_part[q, pl.ds(spare + g, 1), :] = jnp.sum(flows, axis=0, keepdims=True)
        r.projected[q, :, at] = total
        return 0

    for q in range(seqs):
        r.gram[q] = product(r.b_all[q], r.c_all[q], 1, 1)
    backward_first = links.reserve(chunk_total)

    def backward_slot(i, _):
        backward_pair(i, 0)
        c = i - 2 * (seq_count - 1 - s)

        @pl.when((c >= 0) & (c < chunk_total))
        def _():
            hop(r.adj_in, r.state_local, r.adj_out, backward_first, c, False)

        return 0

    slots = chunk_total + 2 * (seq_count - 1)
    assert slots <= pair_total, slots
    lax.fori_loop(0, 5, backward_slot, 0)
    branch_last = spread_over(r.branch, r.branch_near, r.sent, r.branch_far, branch_copies)
    lax.fori_loop(5, 8, backward_slot, 0)
    stream_a(gate_streams[0])
    lax.fori_loop(8, pair_total, backward_slot, 0)

    for q in range(seqs):
        pairs = r.pair_weight[q].astype(LOW)
        d_in = product(pairs, r.c_all[q]) + product(r.weighted_tail[q], r.adj_in[q])
        d_out = product(pairs, r.b_all[q], 0, 0) + product(r.d_growth[q], r.state_in[q])
        r.sel_keep[q] = jnp.where(upper, d_out, d_in)
        r.sel_send[q] = jnp.where(upper, d_in, d_out).astype(LOW)
    sel_over = links.copy(r.sel_send, r.sel_over, {HEAD: over})
    sel_over.start()

    for q in range(seqs):
        running = r.running[q]
        tail = picked(jnp.exp(running[rows - 1 : rows, :] - running), r.expand[...], count=2)
        r.mixed[q] = product(r.b_all[q], r.adj_in[q], 1, 1) * tail

    def value_back(i, _):
        q, base = i // (rows // tile), lax.rem(i, rows // tile) * tile
        at = block(base, tile)
        inter_back = r.mixed[q, at, :]
        projected = r.projected[q, at, :] + inter_back
        step_x = r.step_x[q, at, :]
        d_mixed = r.d_mixed_low[q, at, :].astype(WIDE)
        act = r.act[q, at, :].astype(WIDE)
        d_value = projected * step_x + r.skip_x[0:1, :] * d_mixed
        conv = convolve(r.value_ext, q, base, tile, r.conv_value, value_bias)
        logistic = sigmoid(conv)
        r.slope_v[q, at, :] = d_value * (logistic * (1.0 + conv * (1.0 - logistic)))
        r.projected[q, at, :] = act * projected
        r.mixed[q, at, :] = act * step_x * inter_back
        r.inter[q, at, :] = d_mixed * r.inter[q, at, :]
        return 0

    lax.fori_loop(0, total_rows // tile, value_back, 0)
    rim_back = []
    for q in range(seqs):
        rim_back.append(
            links.copy(
                r.slope_v.at[q, 0:RIM, :],
                r.slope_v.at[q, rows : rows + RIM, :],
                {SEQ: lax.rem(s + seq_count - 1, seq_count)},
            )
        )

    @pl.when(s > 0)
    def _():
        for copy in rim_back:
            copy.start()

    sel_over.wait()
    r.sel_pair[...] = (r.sel_keep[...] + r.sel_over[...].astype(WIDE)).astype(LOW)
    sel_side = links.copy(r.sel_pair, r.sel_side, {HEAD: side})
    sel_side.start()


    sel_side.wait()
    for q in range(seqs):
        total = r.sel_pair[q].astype(WIDE) + r.sel_side[q].astype(WIDE)
        conv = convolve(r.select_ext, q, 0, rows, r.taps, r.taps[4:5, :])
        logistic = sigmoid(conv)
        r.slope_s[q, 0:rows, :] = jnp.where(
            mine, total * (logistic * (1.0 + conv * (1.0 - logistic))), 0.0
        )
    rim_back_s = []
    for q in range(seqs):
        rim_back_s.append(
            links.copy(
                r.slope_s.at[q, 0:RIM, :],
                r.slope_s.at[q, rows : rows + RIM, :],
                {SEQ: lax.rem(s + seq_count - 1, seq_count)},
            )
        )

    @pl.when(s > 0)
    def _():
        for copy in rim_back_s:
            copy.start()

    @pl.when(s < seq_count - 1)
    def _():
        for copy in rim_back:
            copy.wait_recv()

    def conv_back(i, carry):
        q, base = i // (rows // tile), lax.rem(i, rows // tile) * tile
        at = block(base, tile)
        slopes = r.slope_v[q, pl.ds(pl.multiple_of(base, 8), tile + RIM), :]
        wide = r.value_ext[q, pl.ds(pl.multiple_of(base, 8), tile + RIM), :]
        grad = r.conv_value[0:1, :] * slopes[3 : 3 + tile]
        for k in range(1, 4):
            grad = grad + r.conv_value[k : k + 1, :] * slopes[3 - k : 3 - k + tile]
        r.gate[block(i * tile, tile), :] = grad.astype(LOW)
        own = slopes[0:tile]
        fresh = []
        for k in range(4):
            term = own * wide[RIM - 3 + k : RIM - 3 + k + tile]
            total = carry[k]
            for t in range(tile // 8):
                total = total + term[t * 8 : t * 8 + 8]
            fresh.append(total)
        total = carry[4]
        for t in range(tile // 8):
            total = total + own[t * 8 : t * 8 + 8]
        return tuple(fresh) + (total,)

    totals = lax.fori_loop(0, total_rows // tile, conv_back, (blank,) * 5)
    for k in range(5):
        small[k : k + 1, 0:inner] = jnp.sum(totals[k], axis=0, keepdims=True)
    big_grad(r.part_value, r.normed, r.gate[...], piece)
    value_streams = [stream_start(bufs_value, c) for c in range(r.up_value.shape[0])]
    stream_a(gate_streams[1])
    stream_b(gate_streams[0])

    for q in range(seqs):
        step = r.step[q]
        rate = -jnp.exp(r.taps[6:7, :])
        expand = r.expand[...]
        direct = picked(r.projected[q], expand, 1, 1, 2)
        later = picked(r.inter[q], expand, 1, 1, 2)
        earlier = picked(r.mixed[q], expand, 1, 1, 2)
        crossing = r.state_in[q].astype(WIDE) * r.adj_in[q].astype(WIDE)
        bound = picked(picked_by(jnp.ones((8, state), LOW), crossing, 1, 1), expand, 1, 1)[0:1, :]
        last = r.running[q, rows - 1 : rows, :]
        d_log = (
            picked_by(tri[...], later - r.row_part[q], 0, 0)
            + picked_by(tri[...], r.col_part[q], 0, 1)
            + (picked_by(tri[...], earlier) - earlier)
            + bound * jnp.exp(last)
        )
        used = (head_lane >= spare) & (head_lane < spare + heads)
        d_step = direct + d_log * rate
        d_raw = jnp.where(used, d_step * sigmoid(r.step_arg[q]), 0.0)
        r.step_grad[q] = d_raw
        lanes = slice(inner + state, inner + 2 * state)
        small[0:1, lanes] += jnp.sum(d_raw, axis=0, keepdims=True)
        small[1:2, lanes] += jnp.where(used, jnp.sum(d_log * step, axis=0, keepdims=True) * rate, 0.0)


    @pl.when(s < seq_count - 1)
    def _():
        for copy in rim_back_s:
            copy.wait_recv()

    for q in range(seqs):
        slopes = r.slope_s[q]
        wide = r.select_ext[q]
        at = slice(inner, inner + state)
        grad = r.taps[0:1, :] * slopes[3 : 3 + rows]
        for k in range(1, 4):
            grad = grad + r.taps[k : k + 1, :] * slopes[3 - k : 3 - k + rows]
        own = slopes[0:rows]
        for k in range(4):
            small[k : k + 1, at] += jnp.sum(
                own * wide[RIM - 3 + k : RIM - 3 + k + rows], axis=0, keepdims=True
            )
        small[4:5, at] += jnp.sum(own, axis=0, keepdims=True)
        r.select_low[pl.ds(q * rows, rows), :] = jnp.where(mine, grad, r.step_grad[q]).astype(LOW)
    big_grad(r.part_select, r.select_low, r.normed[...], state)
    select_stream = stream_start(bufs_select, 0)
    stream_a(out_streams[0])
    stream_b(gate_streams[1])
    stream_c(gate_streams[0])

    branch_last.wait()

    def output_rows(i, _):
        at = block(i * 64, 64)
        total = (
            r.branch[h, at, :].astype(WIDE)
            + r.branch_near[0, at, :].astype(WIDE)
            + r.branch_far[at, :].astype(WIDE)
        )
        r.o_block[at, :] = (r.x_all[h, at, :].astype(WIDE) + total).astype(LOW)
        return 0

    lax.fori_loop(0, total_rows // 64, output_rows, 0)
    for k in range(head_count):
        columns = slice(k * piece, (k + 1) * piece)

        def d_normed_rows(q, _):
            at = block(q * rows, rows)
            total = product(r.gate_low[at, :], r.v_w_gate[columns, :], 1, 1)
            total = total + product(r.gate[at, :], r.v_w_value[columns, :], 1, 1)
            total = total + product(r.select_low[at, :], r.v_w_select[:, columns])
            mean = jnp.sum(
                total * r.x_all[k, at, :].astype(WIDE) * r.gain_all[k, 0:1, :],
                axis=1,
                keepdims=True,
            )
            r.branch[k, at, :] = total.astype(LOW)
            if k == 0:
                r.sums[at, :] = jnp.where(iota((rows, state), 1) == 0, mean, 0.0)
            else:
                r.sums[at, :] += jnp.where(iota((rows, state), 1) == 0, mean, 0.0)
            return 0

        lax.fori_loop(0, seqs, d_normed_rows, 0)
    normed_copies = spread_parts(r.branch, r.normed_near)
    mean_copies = row_sums(r.mean_own, r.mean_held)
    stream_a(out_streams[1])
    stream_b(out_streams[0])
    stream_c(gate_streams[1])
    normed_last = spread_over(r.branch, r.normed_near, r.sent, r.normed_far, normed_copies)
    row_sums_end(r.mean_own, r.mean_held, mean_copies)
    normed_last.wait()

    def input_rows(i, total):
        at = block(i * 32, 32)
        grad = (
            r.branch[h, at, :].astype(WIDE)
            + r.normed_near[0, at, :].astype(WIDE)
            + r.normed_far[at, :].astype(WIDE)
        )
        own = r.x_all[h, at, :].astype(WIDE)
        inverse = r.inverse[at, 0:1]
        mean = r.sums[at, 0:1] / model
        r.o_input[at, :] = (
            r.cot_all[h, at, :].astype(WIDE)
            + inverse * (grad * r.gain_all[h, 0:1, :])
            - own * (inverse * inverse * inverse * mean)
        )
        term = grad * own * inverse
        for t in range(4):
            total = total + term[t * 8 : t * 8 + 8]
        return total

    gain_grad = lax.fori_loop(0, total_rows // 32, input_rows, jnp.zeros((8, piece), WIDE))
    small[7:8, 0:piece] = jnp.sum(gain_grad, axis=0, keepdims=True)

    small_copies = []
    for j in range(1, seq_count):
        copy = links.copy(small, r.small_seq.at[j - 1], {SEQ: lax.rem(s + j, seq_count)})
        copy.start()
        small_copies.append(copy)
    stream_a(value_streams[0])
    stream_b(out_streams[1])
    stream_c(out_streams[0])
    stream_a(value_streams[1])
    stream_b(value_streams[0])
    stream_c(out_streams[1])
    stream_a(select_stream)
    stream_b(value_streams[1])
    stream_b(select_stream)
    stream_c(value_streams[0])
    stream_c(value_streams[1])
    stream_c(select_stream)
    total = small[...]
    for j, copy in enumerate(small_copies):
        copy.wait()
    for j in range(seq_count - 1):
        total = total + r.small_seq[j]
    r.small_mid[...] = total
    small_copies = []
    for j in range(1, dp_count):
        copy = links.copy(r.small_mid, r.small_dp.at[j - 1], {DP: lax.rem(d + j, dp_count)})
        copy.start()
        small_copies.append(copy)
    for copy in small_copies:
        copy.wait()
    for j in range(dp_count - 1):
        total = total + r.small_dp[j]
    r.o_small[:, 0:inner] = total[:, 0:inner]
    taps_grad, by_head = total[:, inner : inner + state], total[:, inner + state :]
    r.o_small[:, inner : inner + state] = jnp.where(odd, pltpu.roll(taps_grad, half, 1), taps_grad)
    r.o_small[:, inner + state :] = jnp.where(odd, by_head, pltpu.roll(by_head, half, 1))
    for me in keeps:
        stream_d(me)

    @pl.when(s > 0)
    def _():
        for copy in rim_back + rim_back_s:
            copy.wait_send()
        for c in range(chunk_total):
            hop_copy(r.adj_in, r.adj_out, backward_first, c, False)[1].wait_send()

    assert links.count <= size.links, links.count


def finish_kernel(half, heads, piece, inner, *refs):
    ins, outs = refs[:7], refs[7:]
    for source, target in zip(ins[:5], outs[:5]):
        target[...] = source[...].astype(target.dtype)
    matrix, small = ins[5:]
    g_select, g_step, g_norm, g_conv, g_bias, g_conv_s, g_bias_s, g_bias_h, g_decay, g_skip, g_gain = outs[5:]

    @pl.when(pl.program_id(0) == 0)
    def _():
        odd = lax.rem(lax.axis_index(HEAD), 2) == 1
        low_rows, high_rows = matrix[0:half, :].astype(WIDE), matrix[half : 2 * half, :].astype(WIDE)
        g_select[...] = jnp.where(odd, high_rows, low_rows)
        g_step[...] = jnp.where(odd, low_rows, high_rows)[0:heads, :]
        g_norm[...] = small[7:8, 0:piece]
        g_conv[...] = small[0:4, 0:inner]
        g_bias[...] = small[4:5, 0:inner]
        g_gain[...] = small[5:6, 0:inner]
        g_conv_s[...] = small[0:4, inner : inner + half]
        g_bias_s[...] = small[4:5, inner : inner + half]
        for row, target in enumerate((g_bias_h, g_decay, g_skip)):
            target[...] = small[row : row + 1, inner + 2 * half : inner + 2 * half + heads]


def body(size, *args):
    (
        block_input,
        norm_gain,
        w_gate,
        w_value,
        w_select,
        w_step,
        conv_value,
        bias_value,
        conv_select,
        bias_select,
        step_bias,
        decay_log,
        skip_gain,
        gate_gain,
        w_out,
        out_cotangent,
    ) = args
    seqs, rows, piece = block_input.shape
    heads, inner = skip_gain.shape[0], w_value.shape[1]
    head_axis, seq_axis, dp_axis = size[HEAD], size[SEQ], size[DP]
    half = w_select.shape[1]
    state = half * head_axis // 2
    width = inner // heads
    model = piece * head_axis
    total_rows = seqs * rows
    assert head_axis == 4 and seq_axis == 4 and 2 * half == state and heads <= half and 2 * width == state

    def aligned(values):
        values = values.astype(WIDE)
        return jnp.pad(values, (0, -values.shape[0] % state))

    singles = (bias_value, gate_gain, norm_gain, bias_select, step_bias, decay_log, skip_gain)
    singles = [aligned(values) for values in singles]
    starts = [0]
    for values in singles:
        starts.append(starts[-1] + values.shape[0])
    vec = jnp.concatenate(singles)[None]
    vmem = pl.BlockSpec(memory_space=pltpu.VMEM)
    anywhere = pl.BlockSpec(memory_space=pl.ANY)
    inputs = dict(
        x=(block_input.reshape(total_rows, piece), anywhere),
        cot=(out_cotangent.reshape(total_rows, piece), anywhere),
        vec=(vec, vmem),
        conv_value=(conv_value, vmem),
        conv_select=(conv_select, vmem),
        w_select=(w_select.T, vmem),
        w_step=(w_step.T, vmem),
        w_value=(w_value, anywhere),
        w_gate=(w_gate, anywhere),
        w_out=(w_out, anywhere),
    )
    small_shape = (8, inner + 2 * state)

    def result(shape, kind, spec):
        return (jax.ShapeDtypeStruct(shape, kind), spec)

    outputs = dict(
        o_block=result((total_rows, piece), LOW, vmem),
        o_input=result((total_rows, piece), WIDE, vmem),
        o_small=result(small_shape, WIDE, vmem),
        out_out=result((inner, model), LOW, anywhere),
        out_gate=result((model, inner), LOW, anywhere),
        out_value=result((model, inner), LOW, anywhere),
        out_select=result((state, model), LOW, anywhere),
    )
    link_total = 112 + 16 * dp_axis

    def wide(*shape):
        return pltpu.VMEM(shape, WIDE)

    def low(*shape):
        return pltpu.VMEM(shape, LOW)

    def wide_tokens(lanes, extra=0):
        return wide(seqs, rows + extra, lanes)

    def low_tokens(lanes):
        return low(seqs, rows, lanes)

    def over_of(chunks, depth, columns):
        return low(chunks, dp_axis - 1, depth // (chunks * dp_axis), columns)

    def cut_of(chunks, depth, columns):
        return low(chunks, depth // (chunks * dp_axis), columns)

    semaphores = pltpu.SemaphoreType.DMA
    scratch = dict(
        send_sem=semaphores((link_total,)),
        recv_sem=semaphores((link_total,)),
        load_sem=semaphores((5,)),
        keep_sem=semaphores((7,)),
        v_w_select=low(state, model),
        v_w_value=low(model, inner),
        v_w_gate=low(model, inner),
        v_w_out=low(inner, model),
        gain_all=wide(head_axis, 8, piece),
        x_all=low(head_axis, total_rows, piece),
        cot_all=low(head_axis, total_rows, piece),
        normed=low(total_rows, model),
        inverse=wide(total_rows, state),
        expand=low(state, inner),
        tri=low(rows, rows),
        taps=wide(8, state),
        step_arg=wide_tokens(state),
        step=wide_tokens(state),
        running=wide_tokens(state),
        row_part=wide_tokens(state),
        step_grad=wide_tokens(state),
        sel_keep=wide_tokens(state),
        running_t=wide(seqs, state, rows),
        col_part=wide(seqs, state, rows),
        running_x=wide_tokens(heads * state),
        step_x=wide_tokens(inner),
        scale_x=wide_tokens(inner),
        mixed=wide_tokens(inner),
        inter=wide_tokens(inner),
        projected=wide_tokens(inner),
        act=low_tokens(inner),
        weighted=low_tokens(inner),
        weighted_tail=low_tokens(inner),
        d_mixed_low=low_tokens(inner),
        d_growth=low_tokens(inner),
        value_ext=wide_tokens(inner, RIM),
        select_ext=wide_tokens(state, RIM),
        slope_v=wide_tokens(inner, RIM),
        slope_s=wide_tokens(state, RIM),
        select_own=low_tokens(state),
        select_side=low_tokens(state),
        select_pair=low_tokens(state),
        select_over=low_tokens(state),
        b_all=low_tokens(state),
        c_all=low_tokens(state),
        sel_send=low_tokens(state),
        sel_over=low_tokens(state),
        sel_pair=low_tokens(state),
        sel_side=low_tokens(state),
        gram=wide(seqs, rows, rows),
        pair_weight=wide(seqs, rows, rows),
        state_local=wide(seqs, inner, state),
        decay_row=wide(seqs, inner, state),
        state_in=low(seqs, inner, state),
        state_out=low(seqs, inner, state),
        adj_in=low(seqs, inner, state),
        adj_out=low(seqs, inner, state),
        gate=low(total_rows, inner),
        hidden=low(total_rows, inner),
        gate_low=low(total_rows, inner),
        select_low=low(total_rows, state),
        skip_x=wide(8, inner),
        sums=wide(total_rows, state),
        sum_own=wide(8, total_rows),
        sum_held=wide(head_axis - 1, 8, total_rows),
        mean_own=wide(8, total_rows),
        mean_held=wide(head_axis - 1, 8, total_rows),
        branch=low(head_axis, total_rows, piece),
        sent=low(total_rows, piece),
        branch_near=low(2, total_rows, piece),
        branch_far=low(total_rows, piece),
        normed_near=low(2, total_rows, piece),
        normed_far=low(total_rows, piece),
        small=wide(*small_shape),
        small_mid=wide(*small_shape),
        small_seq=wide(seq_axis - 1, *small_shape),
        small_dp=wide(dp_axis - 1, *small_shape),
        part_gate=low(model, inner),
        part_value=low(model, inner),
        part_select=low(state, model),
        over_out=over_of(2, inner, model),
        over_gate=over_of(2, model, inner),
        over_value=over_of(2, model, inner),
        over_select=over_of(1, state, model),
        up_out=cut_of(2, inner, model),
        up_gate=cut_of(2, model, inner),
        up_value=cut_of(2, model, inner),
        up_select=cut_of(1, state, model),
        mid_out=cut_of(2, inner, model),
        mid_gate=cut_of(2, model, inner),
        mid_value=cut_of(2, model, inner),
        mid_select=cut_of(1, state, model),
    )
    facts = SimpleNamespace(
        names=list(inputs) + list(outputs) + list(scratch),
        seqs=seqs,
        rows=rows,
        heads=heads,
        width=width,
        inner=inner,
        state=state,
        piece=piece,
        head_axis=head_axis,
        seq_axis=seq_axis,
        dp_axis=dp_axis,
        links=link_total,
        norm_at=starts[2],
        select_at=starts[3],
        bias_at=starts[4],
        decay_at=starts[5],
        skip_at=starts[6],
    )
    results = pl.pallas_call(
        functools.partial(mixer_kernel, facts),
        out_shape=[shape for shape, _ in outputs.values()],
        in_specs=[spec for _, spec in inputs.values()],
        out_specs=[spec for _, spec in outputs.values()],
        scratch_shapes=list(scratch.values()),
        compiler_params=pltpu.CompilerParams(
            collective_id=0, has_side_effects=True, vmem_limit_bytes=67043328
        ),
    )(*[value for value, _ in inputs.values()])
    got = SimpleNamespace(**dict(zip(outputs, results, strict=True)))
    steps = 8

    def by_rows(depth, columns):
        return pl.BlockSpec((depth // steps, columns), lambda i: (i, 0))

    def whole(*shape):
        return pl.BlockSpec(shape, lambda i: (0, 0))

    streamed = [(total_rows, piece), (total_rows, piece), (inner, model), (model, inner), (model, inner)]
    kinds = [LOW, WIDE, WIDE, WIDE, WIDE]
    fixed = [
        (half, model),
        (heads, model),
        (1, piece),
        (4, inner),
        (1, inner),
        (4, half),
        (1, half),
        (1, heads),
        (1, heads),
        (1, heads),
        (1, inner),
    ]
    final = pl.pallas_call(
        functools.partial(finish_kernel, half, heads, piece, inner),
        grid=(steps,),
        out_shape=[jax.ShapeDtypeStruct(shape, kind) for shape, kind in zip(streamed, kinds)]
        + [jax.ShapeDtypeStruct(shape, WIDE) for shape in fixed],
        in_specs=[by_rows(*shape) for shape in streamed]
        + [whole(state, model), whole(*small_shape)],
        out_specs=[by_rows(*shape) for shape in streamed] + [whole(*shape) for shape in fixed],
    )(
        got.o_block,
        got.o_input,
        got.out_out,
        got.out_gate,
        got.out_value,
        got.out_select,
        got.o_small,
    )
    block_output, input_grad, g_out, g_gate, g_value, g_select, g_step = final[:7]
    g_norm, g_conv, g_bias, g_conv_s, g_bias_s, g_step_bias, g_decay, g_skip, g_gain = final[7:]
    return (
        block_output.reshape(seqs, rows, piece),
        input_grad.reshape(seqs, rows, piece),
        g_norm[0],
        g_gate,
        g_value,
        g_select.T,
        g_step.T,
        g_conv,
        g_bias[0],
        g_conv_s,
        g_bias_s[0],
        g_step_bias[0],
        g_decay[0],
        g_skip[0],
        g_gain[0],
        g_out,
    )


def solution(mesh):
    columns, single, tokens = P(None, HEAD), P(HEAD), P(DP, SEQ, HEAD)
    in_specs = (
        tokens,
        single,
        columns,
        columns,
        columns,
        columns,
        columns,
        single,
        columns,
        single,
        single,
        single,
        single,
        single,
        P(HEAD, None),
        tokens,
    )
    out_specs = (
        tokens,
        tokens,
        single,
        columns,
        columns,
        columns,
        columns,
        columns,
        single,
        columns,
        single,
        single,
        single,
        single,
        single,
        P(HEAD, None),
    )
    return jax.shard_map(
        functools.partial(body, dict(mesh.shape)),
        mesh=mesh,
        in_specs=in_specs,
        out_specs=out_specs,
        check_vma=False,
    )
```

```python
import functools
from types import SimpleNamespace

import jax
import jax.numpy as jnp
from jax import lax
from jax.experimental import pallas as pl
from jax.experimental.pallas import tpu as pltpu
from jax.sharding import PartitionSpec as P

EPSILON = 1e-05
LOW = jnp.bfloat16
WIDE = jnp.float32
MESH = pl.DeviceIdType.MESH
RIM = 8
NEVER = -1e30
HEAD, SEQ, DP = "head", "seq", "dp"


def product(left, right, left_dim=1, right_dim=0):
    return lax.dot_general(
        left,
        right,
        (((left_dim,), (right_dim,)), ((), ())),
        preferred_element_type=WIDE,
    )


def pieces_of(values, count):
    found = []
    for _ in range(count):
        low = values.astype(LOW)
        found.append(low)
        values = values - low.astype(WIDE)
    return found


def picked(left, table, left_dim=1, table_dim=0, count=3):
    parts = [product(part, table, left_dim, table_dim) for part in pieces_of(left, count)]
    return functools.reduce(jnp.add, parts[::-1])


def picked_by(table, right, table_dim=1, right_dim=0, count=3):
    parts = [product(table, part, table_dim, right_dim) for part in pieces_of(right, count)]
    return functools.reduce(jnp.add, parts[::-1])


def iota(shape, dim):
    return lax.broadcasted_iota(jnp.int32, shape, dim)


def sigmoid(values):
    return 1.0 / (1.0 + jnp.exp(-values))


def softplus(values):
    return jnp.maximum(values, 0.0) + jnp.log1p(jnp.exp(-jnp.abs(values)))


def block(start, size):
    return pl.ds(pl.multiple_of(start, size), size)


class Links:
    def __init__(self, send_sem, recv_sem):
        self.send_sem, self.recv_sem, self.count = send_sem, recv_sem, 0

    def reserve(self, number):
        first = self.count
        self.count += number
        return first

    def copy(self, source, target, where, slot=None):
        slot = self.reserve(1) if slot is None else slot
        return pltpu.make_async_remote_copy(
            src_ref=source,
            dst_ref=target,
            send_sem=self.send_sem.at[slot],
            recv_sem=self.recv_sem.at[slot],
            device_id=where,
            device_id_type=MESH,
        )


def mixer_kernel(size, *refs):
    r = SimpleNamespace(**dict(zip(size.names, refs, strict=True)))
    seqs, rows, heads, width = size.seqs, size.rows, size.heads, size.width
    inner, state, piece = size.inner, size.state, size.piece
    head_count, seq_count, dp_count = size.head_axis, size.seq_axis, size.dp_axis
    inner_total, model = inner * head_count, piece * head_count
    total_rows = seqs * rows
    half = state // 2
    links = Links(r.send_sem, r.recv_sem)
    h, s, d = lax.axis_index(HEAD), lax.axis_index(SEQ), lax.axis_index(DP)
    side, over, across = h ^ 1, h ^ 2, h ^ 3
    place = lax.rem(h, 2) * half
    spare = half - place

    loads = []
    weights = (
        (r.w_value, r.v_w_value),
        (r.w_gate, r.v_w_gate),
        (r.w_out, r.v_w_out),
    )
    for index, (source, target) in enumerate(weights):
        load = pltpu.make_async_copy(source, target, r.load_sem.at[index])
        load.start()
        loads.append(load)

    barrier = pltpu.get_barrier_semaphore()
    peers = [{HEAD: lax.rem(h + j, head_count)} for j in range(1, head_count)]
    peers += [{SEQ: lax.rem(s + j, seq_count)} for j in range(1, seq_count)]
    peers += [{DP: lax.rem(d + j, dp_count)} for j in range(1, dp_count)]
    for peer in peers:
        pl.semaphore_signal(barrier, inc=1, device_id=peer, device_id_type=MESH)
    pl.semaphore_wait(barrier, len(peers))

    def gather_start(own, held):
        near = links.copy(own, held.at[h], {HEAD: side})
        far = links.copy(own, held.at[h], {HEAD: over})
        far.start()
        near.start()
        return (near, far)

    def gather_pass(held, pair):
        pair[1].wait_recv()
        forward = links.copy(held.at[over], held.at[over], {HEAD: side})
        forward.start()
        return pair + (forward,)

    def gather_end(copies):
        copies[0].wait_recv()
        copies[2].wait_recv()
        for copy in copies:
            copy.wait_send()

    r.gain_all[h] = jnp.broadcast_to(r.norm_gain[...][None].astype(WIDE), (8, piece))
    gain_copies = gather_start(r.gain_all.at[h], r.gain_all)
    input_copies = gather_start(r.x, r.x_all)
    cot_copies = gather_start(r.cot, r.cot_all)

    own_x = pltpu.make_async_copy(r.x, r.x_all.at[h], r.load_sem.at[3])
    own_cot = pltpu.make_async_copy(r.cot, r.cot_all.at[h], r.load_sem.at[4])
    own_x.start()
    own_cot.start()

    odd = lax.rem(h, 2) == 1
    r.expand[...] = jnp.where(
        (iota((state, inner), 1) // width + spare) == iota((state, inner), 0), 1.0, 0.0
    ).astype(LOW)
    lower = iota((rows, rows), 0) >= iota((rows, rows), 1)
    r.tri[...] = jnp.where(lower, 1.0, 0.0).astype(LOW)
    shift = jnp.where(iota((half, state), 0) + place == iota((half, state), 1), 1.0, 0.0).astype(LOW)
    r.taps[0:4, :] = picked(r.conv_select[...], shift)
    few = jnp.broadcast_to(r.bias_select[...][None], (8, half))
    r.taps[4:5, :] = picked(few, shift)[0:1, :]
    moved = jnp.where(
        iota((heads, state), 0) + spare == iota((heads, state), 1), 1.0, 0.0
    ).astype(LOW)
    for row, source in enumerate((r.step_bias, r.decay_log, r.skip_gain)):
        few = jnp.broadcast_to(source[...][None], (8, heads))
        r.taps[5 + row : 6 + row, :] = picked(few, moved)[0:1, :]
    r.v_w_select[...] = jnp.zeros((state, model), LOW)
    r.v_w_select[pl.ds(pl.multiple_of(place, half), half), :] = r.w_select[...]
    padded = jnp.concatenate([r.w_step[...], jnp.zeros((16 - heads, model), LOW)], axis=0)
    r.v_w_select[pl.ds(pl.multiple_of(spare, half), 16), :] = padded

    @pl.when(s == 0)
    def _():
        r.value_ext[:, 0:RIM, :] = jnp.zeros((seqs, RIM, inner), WIDE)
        r.select_ext[:, 0:RIM, :] = jnp.zeros((seqs, RIM, state), WIDE)
        r.state_in[...] = jnp.zeros((seqs, inner, state), LOW)

    @pl.when(s == seq_count - 1)
    def _():
        r.slope_v[:, rows : rows + RIM, :] = jnp.zeros((seqs, RIM, inner), WIDE)
        r.slope_s[:, rows : rows + RIM, :] = jnp.zeros((seqs, RIM, state), WIDE)
        r.adj_in[...] = jnp.zeros((seqs, inner, state), LOW)

    gain_copies = gather_pass(r.gain_all, gain_copies)
    input_copies = gather_pass(r.x_all, input_copies)
    gather_end(gain_copies)
    gather_end(input_copies)
    own_x.wait()

    def norm_rows(i, _):
        at = block(i * 64, 64)
        total = jnp.zeros((64, 1), WIDE)
        for k in range(head_count):
            part = r.x_all[k, at, :].astype(WIDE)
            total = total + jnp.sum(part * part, axis=1, keepdims=True)
        inverse = lax.rsqrt(total / model + EPSILON)
        r.inverse[at, :] = jnp.broadcast_to(inverse, (64, state))
        for k in range(head_count):
            part = r.x_all[k, at, :].astype(WIDE)
            r.normed[at, k * piece : (k + 1) * piece] = (
                part * inverse * r.gain_all[k, 0:1, :]
            ).astype(LOW)
        return 0

    lax.fori_loop(0, total_rows // 64, norm_rows, 0)

    paired = dp_count == 2
    mate = {DP: lax.rem(d + 1, dp_count)}
    wide_half = model // 2
    own_half = pl.ds(pl.multiple_of(lax.rem(d, 2) * wide_half, 128), wide_half)
    mate_half = pl.ds(pl.multiple_of(lax.rem(d + 1, 2) * wide_half, 128), wide_half)
    halves = head_count // 2

    def chunk_sends(source, target):
        chunks, _, lanes = target.shape
        copies = []
        for c in range(chunks):
            at = slice(c * lanes, (c + 1) * lanes)
            copies.append(links.copy(source.at[:, at], target.at[c], mate))
            copies[-1].start()
        return copies

    if paired:
        send_normed = links.copy(r.normed.at[:, mate_half], r.far_normed, mate)
        send_normed.start()

    for q in range(seqs):
        at = pl.ds(q * rows, rows)
        both = product(r.normed[at, :], r.v_w_select[...], 1, 1)
        r.step_arg[q] = both + r.taps[5:6, :]
        r.select_ext[q, RIM : RIM + rows, :] = both.astype(LOW).astype(WIDE)
    loads[0].wait()

    def value_matmul(q, _):
        at = block(q * rows, rows)
        r.value_ext[q, RIM : RIM + rows, :] = (
            product(r.normed[at, :], r.v_w_value[...]).astype(LOW).astype(WIDE)
        )
        return 0

    lax.fori_loop(0, seqs, value_matmul, 0)
    rims = []
    for ext in (r.select_ext, r.value_ext):
        for q in range(seqs):
            rims.append(
                links.copy(
                    ext.at[q, rows : rows + RIM, :],
                    ext.at[q, 0:RIM, :],
                    {SEQ: lax.rem(s + 1, seq_count)},
                )
            )

    @pl.when(s < seq_count - 1)
    def _():
        for copy in rims:
            copy.start()

    cot_copies = gather_pass(r.cot_all, cot_copies)

    tri = r.tri
    for q in range(seqs):
        step = softplus(r.step_arg[q])
        r.step[q] = step
        rate = -jnp.exp(r.taps[6:7, :])
        fall = step * rate
        running = picked_by(tri[...], fall)
        r.running[q] = running
        r.running_t[q] = picked(fall, tri[...], 0, 1)

        def spread(g, _):
            lanes = 4 * state
            pick = jnp.where(
                iota((state, lanes), 0) == spare + 4 * g + iota((state, lanes), 1) // state, 1.0, 0.0
            ).astype(LOW)
            r.running_x[q, :, block(g * lanes, lanes)] = picked(r.running[q], pick)
            return 0

        lax.fori_loop(0, heads // 4, spread, 0)
        r.step_x[q] = picked(step, r.expand[...], count=2)
        last = running[rows - 1 : rows, :]
        r.scale_x[q] = picked(jnp.exp(last - running), r.expand[...], count=2)
        decay = jnp.broadcast_to(jnp.exp(r.running_t[q, :, rows - 1 : rows]), (state, state))
        r.decay_row[q] = picked_by(r.expand[...], decay, 0, 0, count=2)

    @pl.when(s > 0)
    def _():
        for copy in rims:
            copy.wait_recv()

    @pl.when(s < seq_count - 1)
    def _():
        for copy in rims:
            copy.wait_send()

    lane_row = iota((1, state), 1)
    mine = (lane_row >= place) & (lane_row < place + half)

    def convolve(ext, q, base, count, taps, bias):
        wide = ext[q, pl.ds(pl.multiple_of(base, 8), count + RIM), :]
        total = bias
        for k in range(4):
            total = total + taps[k : k + 1, :] * wide[RIM - 3 + k : RIM - 3 + k + count]
        return total

    value_bias, gate_gain = r.bias_value[...][None], r.gate_gain[...][None]

    for q in range(seqs):
        conv = convolve(r.select_ext, q, 0, rows, r.taps, r.taps[4:5, :])
        act = jnp.where(mine, conv * sigmoid(conv), 0.0)
        r.select_own[q] = act.astype(LOW)
    pair = links.copy(r.select_own, r.select_side, {HEAD: side})
    pair.start()

    def value_conv(i, _):
        q, base = i // (rows // 64), lax.rem(i, rows // 64) * 64
        conv = convolve(r.value_ext, q, base, 64, r.conv_value, value_bias)
        act = (conv * sigmoid(conv)).astype(LOW)
        at = block(base, 64)
        r.act[q, at, :] = act
        r.weighted[q, at, :] = (act.astype(WIDE) * r.step_x[q, at, :]).astype(LOW)
        return 0

    lax.fori_loop(0, seqs * (rows // 64), value_conv, 0)
    pair.wait()
    r.select_pair[...] = r.select_own[...] + r.select_side[...]
    swap = links.copy(r.select_pair, r.select_over, {HEAD: over})
    swap.start()
    loads[1].wait()

    def gate_matmul(q, _):
        at = block(q * rows, rows)
        r.gate[at, :] = product(r.normed[at, :], r.v_w_gate[...]).astype(LOW)
        return 0

    lax.fori_loop(0, seqs, gate_matmul, 0)
    swap.wait()
    gather_end(cot_copies)
    own_cot.wait()
    if paired:
        at = pl.ds(lax.rem(d + 1, 2) * halves, halves)
        send_cot = links.copy(r.cot_all.at[at], r.far_cot, mate)
        send_cot.start()
    upper = h >= 2
    first, second = r.select_pair[...], r.select_over[...]
    r.b_all[...] = jnp.where(upper, second, first)
    r.c_all[...] = jnp.where(upper, first, second)

    for q in range(seqs):
        b = r.b_all[q]
        tailed = (r.weighted[q].astype(WIDE) * r.scale_x[q]).astype(LOW)
        r.weighted_tail[q] = tailed
        r.state_local[q] = product(tailed, b, 0, 0)
        r.gram[q] = product(r.c_all[q], b, 1, 1)
        r.scale_x[q] = picked(jnp.exp(r.running[q]), r.expand[...], count=2)

    chunk_rows = inner // 3

    chunk_total = 3 * seqs

    def hop_copy(held, sent, first, c, forward):
        at = pl.ds(pl.multiple_of(lax.rem(c, 3) * chunk_rows, 16), chunk_rows)
        to = lax.rem(s + (1 if forward else seq_count - 1), seq_count)
        return at, links.copy(sent.at[c // 3, at, :], held.at[c // 3, at, :], {SEQ: to}, first + c)

    def hop(held, local, sent, first, c, forward):
        q = c // 3
        at, copy = hop_copy(held, sent, first, c, forward)

        @pl.when((s > 0) if forward else (s < seq_count - 1))
        def _():
            copy.wait_recv()

        sent[q, at, :] = (
            local[q, at, :] + r.decay_row[q, at, :] * held[q, at, :].astype(WIDE)
        ).astype(LOW)

        @pl.when((s < seq_count - 1) if forward else (s > 0))
        def _():
            copy.start()

    half_lane = iota((rows, state), 1) < width

    def decay_of(q, g):
        column = r.running_x[q, :, block(g * state, state)]
        gap = jnp.concatenate([column] * (rows // state), axis=1) - r.running_t[q, pl.ds(spare + g, 1), :]
        return jnp.exp(jnp.where(lower, gap, NEVER))

    def forward_pair(i, _):
        q, j = i // (heads // 2), lax.rem(i, heads // 2)
        at = block(j * state, state)
        values = r.weighted[q, :, at]
        zero = jnp.zeros_like(values)
        total = jnp.zeros((rows, state), WIDE)
        for part in range(2):
            mixing = (r.gram[q] * decay_of(q, 2 * j + part)).astype(LOW)
            kept = jnp.where(half_lane if part == 0 else ~half_lane, values, zero)
            total = total + product(mixing, kept)
        r.mixed[q, :, at] = total
        return 0

    pair_total = seqs * heads // 2
    forward_first = links.reserve(chunk_total)

    def forward_slot(i, _):
        @pl.when(i < pair_total)
        def _():
            forward_pair(i, 0)

        c = i - chunk_total * s

        @pl.when((c >= 0) & (c < chunk_total))
        def _():
            hop(r.state_in, r.state_local, r.state_out, forward_first, c, True)

        return 0

    lax.fori_loop(0, pair_total, forward_slot, 0)
    loads[2].wait()

    def d_hidden_matmul(q, _):
        at = block(q * rows, rows)
        total = product(r.cot_all[0, at, :], r.v_w_out[:, 0:piece], 1, 1)
        for k in range(1, head_count):
            total = total + product(
                r.cot_all[k, at, :], r.v_w_out[:, k * piece : (k + 1) * piece], 1, 1
            )
        r.projected[q] = total
        return 0

    lax.fori_loop(0, seqs, d_hidden_matmul, 0)
    lax.fori_loop(pair_total, max(pair_total, chunk_total * seq_count), forward_slot, 0)

    r.skip_x[...] = picked(jnp.broadcast_to(r.taps[7:8, :], (8, state)), r.expand[...])
    for q in range(seqs):
        r.inter[q] = product(r.c_all[q], r.state_in[q], 1, 1) * r.scale_x[q]

    tile = 32
    lanes_tile = iota((tile, state), 1)

    def gate_rows(i, _):
        q, base = i // (rows // tile), lax.rem(i, rows // tile) * tile
        at, flat = block(base, tile), block(i * tile, tile)
        mixed = (
            r.mixed[q, at, :]
            + r.inter[q, at, :]
            + r.skip_x[0:1, :] * r.act[q, at, :].astype(WIDE)
        )
        r.mixed[q, at, :] = mixed
        gate = r.gate[flat, :].astype(WIDE)
        gated = mixed * (gate * sigmoid(gate))
        squares = jnp.sum(gated * gated, axis=1, keepdims=True)
        dots = jnp.sum(gated * r.projected[q, at, :] * gate_gain, axis=1, keepdims=True)
        r.sums[flat, :] = jnp.where(lanes_tile == 0, squares, jnp.where(lanes_tile == 1, dots, 0.0))
        return 0

    lax.fori_loop(0, total_rows // tile, gate_rows, 0)
    picks = jnp.where(iota((8, state), 0) == iota((8, state), 1), 1.0, 0.0).astype(LOW)

    def row_sums(own, held):
        own[...] = picked_by(picks, r.sums[...], 1, 1)
        copies = []
        for j in range(1, head_count):
            copy = links.copy(own, held.at[j - 1], {HEAD: h ^ j})
            copy.start()
            copies.append(copy)
        return copies

    def row_sums_end(own, held, copies):
        total = own[...]
        for j, copy in enumerate(copies):
            copy.wait_recv()
            total = total + held[j]
        r.sums[...] = picked(total, picks, 0, 0)
        for copy in copies:
            copy.wait_send()

    sum_copies = row_sums(r.sum_own, r.sum_held)

    @pl.when(s < seq_count - 1)
    def _():
        for c in range(chunk_total):
            hop_copy(r.state_in, r.state_out, forward_first, c, True)[1].wait_send()

    row_sums_end(r.sum_own, r.sum_held, sum_copies)

    small = r.small
    small[...] = jnp.zeros(small.shape, WIDE)

    def norm_back(i, carry):
        gain_total, skip_total = carry
        q, base = i // (rows // tile), lax.rem(i, rows // tile) * tile
        at, flat = block(base, tile), block(i * tile, tile)
        sums = r.sums[flat, :]
        scale = lax.rsqrt(sums[:, 0:1] / inner_total + EPSILON)
        mean = scale * scale * scale * (sums[:, 1:2] / inner_total)
        mixed = r.mixed[q, at, :]
        gate = r.gate[flat, :].astype(WIDE)
        logistic = sigmoid(gate)
        gate_act = gate * logistic
        gated = mixed * gate_act
        normal = gated * scale
        grad = r.projected[q, at, :]
        gain = gate_gain
        r.hidden[flat, :] = (normal * gain).astype(LOW)
        d_gated = scale * (grad * gain) - gated * mean
        d_mixed = d_gated * gate_act
        r.d_mixed_low[q, at, :] = d_mixed.astype(LOW)
        r.d_growth[q, at, :] = (d_mixed * r.scale_x[q, at, :]).astype(LOW)
        r.gate_low[flat, :] = (
            d_gated * mixed * (logistic * (1.0 + gate * (1.0 - logistic)))
        ).astype(LOW)
        gain_part = grad * normal
        skip_part = d_mixed * r.act[q, at, :].astype(WIDE)
        for k in range(tile // 8):
            gain_total = gain_total + gain_part[k * 8 : k * 8 + 8]
            skip_total = skip_total + skip_part[k * 8 : k * 8 + 8]
        return gain_total, skip_total

    blank = jnp.zeros((8, inner), WIDE)
    gain_total, skip_total = lax.fori_loop(0, total_rows // tile, norm_back, (blank, blank))
    small[5:6, 0:inner] = jnp.sum(gain_total, axis=0, keepdims=True)
    lanes = slice(inner + state, inner + 2 * state)
    skip_total = jnp.broadcast_to(jnp.sum(skip_total, axis=0, keepdims=True), (8, inner))
    small[2:3, lanes] = picked(skip_total, r.expand[...], 1, 1)[0:1, :]

    if paired:
        send_hidden = chunk_sends(r.hidden, r.far_hidden)
        send_gate = chunk_sends(r.gate_low, r.far_gate)

    for q in range(seqs):
        r.state_local[q] = product(r.d_growth[q], r.c_all[q], 0, 0)

    ends = (s == 0) | (s == seq_count - 1)
    inside = (s > 0) & (s < seq_count - 1)

    keeps = []

    def stream_links(own, up, mid, target):
        me = SimpleNamespace(own=own, up=up, mid=mid, copies=[])
        me.copy_up = links.copy(own, up, {SEQ: s ^ 1})
        me.copy_mid = links.copy(own, mid, {SEQ: seq_count - 1 - s})
        me.copy_down = links.copy(up, up, {SEQ: s ^ 1})
        me.keep = pltpu.make_async_copy(up, target, r.keep_sem.at[len(keeps)])
        me.copies_out = [
            links.copy(up, target, {DP: lax.rem(d + j, dp_count)}) for j in range(1, dp_count)
        ]
        keeps.append(me)
        return me

    def stream_start(bufs, chunk):
        part, over, up, mid, out = bufs
        depth = up.shape[1]

        def rows_of(p):
            return pl.ds(pl.multiple_of((chunk * dp_count + p) * depth, 16), depth)

        me = stream_links(part.at[rows_of(d), :], up.at[chunk], mid.at[chunk], out.at[rows_of(d), :])
        me.over = over.at[chunk]
        for j in range(1, dp_count):
            to = lax.rem(d + j, dp_count)
            copy = links.copy(part.at[rows_of(to), :], me.over.at[j - 1], {DP: to})
            copy.start()
            me.copies.append(copy)
        return me

    def pair_streams(part, up, mid, out, by_columns):
        made = []
        for chunk in range(up.shape[0]):
            if by_columns:
                depth = up.shape[1]
                target = out.at[chunk * depth : (chunk + 1) * depth, own_half]
            else:
                lanes = up.shape[2]
                first = pl.multiple_of(lax.rem(d, 2) * wide_half, 16)
                target = out.at[pl.ds(first, wide_half), chunk * lanes : (chunk + 1) * lanes]
            made.append(stream_links(part.at[chunk], up.at[chunk], mid.at[chunk], target))
        return made

    def add_rows(first, target, terms):
        depth = target.shape[0]
        step = next(t for t in (64, 48, 16) if depth % t == 0)

        def add(i, _):
            at = pl.ds(pl.multiple_of(i * step, 16), step)
            total = first[at, :].astype(WIDE)
            for term in terms:
                total = total + term[at, :].astype(WIDE)
            target[at, :] = total.astype(LOW)
            return 0

        lax.fori_loop(0, depth // step, add, 0)

    def stream_up(me):
        @pl.when(ends)
        def _():
            me.copy_up.start()

    def stream_a(me):
        for copy in me.copies:
            copy.wait_recv()
        add_rows(me.own, me.own, [me.over.at[j] for j in range(dp_count - 1)])
        stream_up(me)

    def stream_b(me):
        @pl.when(inside)
        def _():
            me.copy_up.wait_recv()
            add_rows(me.own, me.own, [me.up])
            me.copy_mid.start()

    def stream_c(me):
        @pl.when(inside)
        def _():
            me.copy_mid.wait_recv()
            add_rows(me.own, me.up, [me.mid])
            me.copy_down.start()

        @pl.when(ends)
        def _():
            me.copy_down.wait_recv()

        me.keep.start()
        for copy in me.copies_out:
            copy.start()

    def stream_d(me):
        for copy in me.copies_out:
            copy.wait()
        for copy in me.copies:
            copy.wait_send()
        me.keep.wait()

        @pl.when(ends)
        def _():
            me.copy_up.wait_send()

        @pl.when(inside)
        def _():
            me.copy_mid.wait_send()
            me.copy_down.wait_send()

    def pair_grad(part, right, far_right, sends, made):
        lanes = part.shape[2]
        for c, copy in enumerate(sends):
            copy.wait()
            at = slice(c * lanes, (c + 1) * lanes)
            for start in range(0, wide_half, piece):
                first = lax.rem(d, 2) * wide_half + start
                left = r.normed[:, pl.ds(pl.multiple_of(first, 128), piece)]
                total = product(left, right[:, at], 0, 0)
                total = total + product(r.far_normed[:, start : start + piece], far_right[c], 0, 0)
                part[c, start : start + piece, :] = total.astype(LOW)
            stream_up(made[c])

    def out_grad():
        for c, copy in enumerate(send_hidden):
            copy.wait_recv()
            lanes = r.far_hidden.shape[2]
            for k in range(halves):
                left = r.hidden[:, c * lanes : (c + 1) * lanes]
                total = product(left, r.cot_all[lax.rem(d, 2) * halves + k], 0, 0)
                total = total + product(r.far_hidden[c], r.far_cot[k], 0, 0)
                r.part_out[c, :, k * piece : (k + 1) * piece] = total.astype(LOW)
            stream_up(out_streams[c])

    def big_grad(part, left, right, lanes):
        for start in range(0, part.shape[0], lanes):
            columns = slice(start, start + lanes)
            part[columns, :] = product(left[:, columns], right, 0, 0).astype(LOW)

    if paired:
        out_streams = pair_streams(r.part_out, r.up_out, r.mid_out, r.out_out, True)
        gate_streams = pair_streams(r.part_gate, r.up_gate, r.mid_gate, r.out_gate, False)
        value_streams = pair_streams(r.part_value, r.up_value, r.mid_value, r.out_value, False)
        select_streams = pair_streams(r.part_select, r.up_select, r.mid_select, r.out_select, True)
    else:
        bufs_gate = (r.part_gate, r.over_gate, r.up_gate, r.mid_gate, r.out_gate)
        bufs_out = (r.part_out, r.over_out, r.up_out, r.mid_out, r.out_out)
        bufs_value = (r.part_value, r.over_value, r.up_value, r.mid_value, r.out_value)
        bufs_select = (r.part_select, r.over_select, r.up_select, r.mid_select, r.out_select)
        big_grad(r.part_gate, r.normed, r.gate_low[...], piece)
        gate_streams = [stream_start(bufs_gate, c) for c in range(r.up_gate.shape[0])]

    def spread_parts(part, near):
        copies = [
            links.copy(part.at[side], near.at[0], {HEAD: side}),
            links.copy(part.at[across], near.at[1], {HEAD: side}),
        ]
        for copy in copies:
            copy.start()
        return copies

    def spread_over(part, near, sent, far, copies):
        for copy in copies:
            copy.wait_recv()

        def add(i, _):
            at = block(i * 64, 64)
            sent[at, :] = (
                part[over, at, :].astype(WIDE) + near[1, at, :].astype(WIDE)
            ).astype(LOW)
            return 0

        lax.fori_loop(0, total_rows // 64, add, 0)
        last = links.copy(sent, far, {HEAD: over})
        last.start()
        for copy in copies:
            copy.wait_send()
        return last

    for k in range(head_count):
        r.branch[k] = product(
            r.hidden[...], r.v_w_out[:, k * piece : (k + 1) * piece]
        ).astype(LOW)
    branch_copies = spread_parts(r.branch, r.branch_near)
    if not paired:
        for k in range(head_count):
            columns = slice(k * piece, (k + 1) * piece)
            r.part_out[:, columns] = product(r.hidden[...], r.cot_all[k], 0, 0).astype(LOW)
        out_streams = [stream_start(bufs_out, c) for c in range(r.up_out.shape[0])]

    r.pair_weight[...] = jnp.zeros((seqs, rows, rows), WIDE)
    r.row_part[...] = jnp.zeros((seqs, rows, state), WIDE)
    r.col_part[...] = jnp.zeros((seqs, state, rows), WIDE)
    head_lane = iota((1, state), 1)

    upper_tri = iota((rows, rows), 0) <= iota((rows, rows), 1)

    def backward_pair(i, _):
        q, j = i // (heads // 2), lax.rem(i, heads // 2)
        at = block(j * state, state)
        grads, values = r.d_mixed_low[q, :, at], r.weighted[q, :, at]
        gram = r.gram[q]
        zero = jnp.zeros_like(grads)
        total = jnp.zeros((rows, state), WIDE)
        for part in range(2):
            g = 2 * j + part
            column = r.running_x[q, :, block(g * state, state)]
            gap = r.running_t[q, pl.ds(spare + g, 1), :] - jnp.concatenate(
                [column] * (rows // state), axis=1
            )
            decay = jnp.exp(jnp.where(upper_tri, gap, NEVER))
            kept = jnp.where(half_lane if part == 0 else ~half_lane, grads, zero)
            total = total + product((gram * decay).astype(LOW), kept)
            pairs = decay * product(values, kept, 1, 1)
            r.pair_weight[q] += pairs
            flows = pairs * gram
            r.row_part[q] += jnp.where(
                head_lane == spare + g, jnp.sum(flows, axis=1, keepdims=True), 0.0
            )
            r.col_part[q, pl.ds(spare + g, 1), :] = jnp.sum(flows, axis=0, keepdims=True)
        r.projected[q, :, at] = total
        return 0

    for q in range(seqs):
        r.gram[q] = product(r.b_all[q], r.c_all[q], 1, 1)
    backward_first = links.reserve(chunk_total)

    def backward_slot(i, _):
        backward_pair(i, 0)
        c = i - 2 * (seq_count - 1 - s)

        @pl.when((c >= 0) & (c < chunk_total))
        def _():
            hop(r.adj_in, r.state_local, r.adj_out, backward_first, c, False)

        return 0

    slots = chunk_total + 2 * (seq_count - 1)
    assert slots <= pair_total, slots
    lax.fori_loop(0, chunk_total, backward_slot, 0)
    branch_last = spread_over(r.branch, r.branch_near, r.sent, r.branch_far, branch_copies)
    if paired:
        send_normed.wait()
        send_cot.wait()

        @pl.when(s == 0)
        def _():
            out_grad()

    lax.fori_loop(chunk_total, pair_total, backward_slot, 0)

    for q in range(seqs):
        pairs = r.pair_weight[q].astype(LOW)
        d_in = product(pairs, r.c_all[q]) + product(r.weighted_tail[q], r.adj_in[q])
        d_out = product(pairs, r.b_all[q], 0, 0) + product(r.d_growth[q], r.state_in[q])
        r.sel_keep[q] = jnp.where(upper, d_out, d_in)
        r.sel_send[q] = jnp.where(upper, d_in, d_out).astype(LOW)
    sel_over = links.copy(r.sel_send, r.sel_over, {HEAD: over})
    sel_over.start()

    for q in range(seqs):
        running = r.running[q]
        tail = picked(jnp.exp(running[rows - 1 : rows, :] - running), r.expand[...], count=2)
        r.mixed[q] = product(r.b_all[q], r.adj_in[q], 1, 1) * tail

    def value_back(i, _):
        q, base = i // (rows // tile), lax.rem(i, rows // tile) * tile
        at = block(base, tile)
        inter_back = r.mixed[q, at, :]
        projected = r.projected[q, at, :] + inter_back
        step_x = r.step_x[q, at, :]
        d_mixed = r.d_mixed_low[q, at, :].astype(WIDE)
        act = r.act[q, at, :].astype(WIDE)
        d_value = projected * step_x + r.skip_x[0:1, :] * d_mixed
        conv = convolve(r.value_ext, q, base, tile, r.conv_value, value_bias)
        logistic = sigmoid(conv)
        r.slope_v[q, at, :] = d_value * (logistic * (1.0 + conv * (1.0 - logistic)))
        r.projected[q, at, :] = act * projected
        r.mixed[q, at, :] = act * step_x * inter_back
        r.inter[q, at, :] = d_mixed * r.inter[q, at, :]
        return 0

    lax.fori_loop(0, total_rows // tile, value_back, 0)
    rim_back = []
    for q in range(seqs):
        rim_back.append(
            links.copy(
                r.slope_v.at[q, 0:RIM, :],
                r.slope_v.at[q, rows : rows + RIM, :],
                {SEQ: lax.rem(s + seq_count - 1, seq_count)},
            )
        )

    @pl.when(s > 0)
    def _():
        for copy in rim_back:
            copy.start()

    if paired:

        @pl.when(s > 0)
        def _():
            out_grad()

    sel_over.wait()
    r.sel_pair[...] = (r.sel_keep[...] + r.sel_over[...].astype(WIDE)).astype(LOW)
    sel_side = links.copy(r.sel_pair, r.sel_side, {HEAD: side})
    sel_side.start()


    sel_side.wait()
    for q in range(seqs):
        total = r.sel_pair[q].astype(WIDE) + r.sel_side[q].astype(WIDE)
        conv = convolve(r.select_ext, q, 0, rows, r.taps, r.taps[4:5, :])
        logistic = sigmoid(conv)
        r.slope_s[q, 0:rows, :] = jnp.where(
            mine, total * (logistic * (1.0 + conv * (1.0 - logistic))), 0.0
        )
    rim_back_s = []
    for q in range(seqs):
        rim_back_s.append(
            links.copy(
                r.slope_s.at[q, 0:RIM, :],
                r.slope_s.at[q, rows : rows + RIM, :],
                {SEQ: lax.rem(s + seq_count - 1, seq_count)},
            )
        )

    @pl.when(s > 0)
    def _():
        for copy in rim_back_s:
            copy.start()

    @pl.when(s < seq_count - 1)
    def _():
        for copy in rim_back:
            copy.wait_recv()

    def conv_back(i, carry):
        q, base = i // (rows // tile), lax.rem(i, rows // tile) * tile
        at = block(base, tile)
        slopes = r.slope_v[q, pl.ds(pl.multiple_of(base, 8), tile + RIM), :]
        wide = r.value_ext[q, pl.ds(pl.multiple_of(base, 8), tile + RIM), :]
        grad = r.conv_value[0:1, :] * slopes[3 : 3 + tile]
        for k in range(1, 4):
            grad = grad + r.conv_value[k : k + 1, :] * slopes[3 - k : 3 - k + tile]
        r.gate[block(i * tile, tile), :] = grad.astype(LOW)
        own = slopes[0:tile]
        fresh = []
        for k in range(4):
            term = own * wide[RIM - 3 + k : RIM - 3 + k + tile]
            total = carry[k]
            for t in range(tile // 8):
                total = total + term[t * 8 : t * 8 + 8]
            fresh.append(total)
        total = carry[4]
        for t in range(tile // 8):
            total = total + own[t * 8 : t * 8 + 8]
        return tuple(fresh) + (total,)

    totals = lax.fori_loop(0, total_rows // tile, conv_back, (blank,) * 5)
    for k in range(5):
        small[k : k + 1, 0:inner] = jnp.sum(totals[k], axis=0, keepdims=True)
    if paired:
        send_value = chunk_sends(r.gate, r.far_value)
        stream_b(out_streams[0])
        stream_b(out_streams[1])
        pair_grad(r.part_gate, r.gate_low, r.far_gate, send_gate, gate_streams)
    else:
        big_grad(r.part_value, r.normed, r.gate[...], piece)
        value_streams = [stream_start(bufs_value, c) for c in range(r.up_value.shape[0])]
        for me in out_streams + gate_streams:
            stream_a(me)
        stream_b(out_streams[0])
        stream_b(out_streams[1])
    stream_c(out_streams[0])
    stream_b(out_streams[2])
    stream_c(out_streams[1])

    for q in range(seqs):
        step = r.step[q]
        rate = -jnp.exp(r.taps[6:7, :])
        expand = r.expand[...]
        direct = picked(r.projected[q], expand, 1, 1, 2)
        later = picked(r.inter[q], expand, 1, 1, 2)
        earlier = picked(r.mixed[q], expand, 1, 1, 2)
        crossing = r.state_in[q].astype(WIDE) * r.adj_in[q].astype(WIDE)
        bound = picked(picked_by(jnp.ones((8, state), LOW), crossing, 1, 1), expand, 1, 1)[0:1, :]
        last = r.running[q, rows - 1 : rows, :]
        d_log = (
            picked_by(tri[...], later - r.row_part[q], 0, 0)
            + picked_by(tri[...], r.col_part[q], 0, 1)
            + (picked_by(tri[...], earlier) - earlier)
            + bound * jnp.exp(last)
        )
        used = (head_lane >= spare) & (head_lane < spare + heads)
        d_step = direct + d_log * rate
        d_raw = jnp.where(used, d_step * sigmoid(r.step_arg[q]), 0.0)
        r.step_grad[q] = d_raw
        lanes = slice(inner + state, inner + 2 * state)
        small[0:1, lanes] += jnp.sum(d_raw, axis=0, keepdims=True)
        small[1:2, lanes] += jnp.where(used, jnp.sum(d_log * step, axis=0, keepdims=True) * rate, 0.0)


    @pl.when(s < seq_count - 1)
    def _():
        for copy in rim_back_s:
            copy.wait_recv()

    for q in range(seqs):
        slopes = r.slope_s[q]
        wide = r.select_ext[q]
        at = slice(inner, inner + state)
        grad = r.taps[0:1, :] * slopes[3 : 3 + rows]
        for k in range(1, 4):
            grad = grad + r.taps[k : k + 1, :] * slopes[3 - k : 3 - k + rows]
        own = slopes[0:rows]
        for k in range(4):
            small[k : k + 1, at] += jnp.sum(
                own * wide[RIM - 3 + k : RIM - 3 + k + rows], axis=0, keepdims=True
            )
        small[4:5, at] += jnp.sum(own, axis=0, keepdims=True)
        r.select_low[pl.ds(q * rows, rows), :] = jnp.where(mine, grad, r.step_grad[q]).astype(LOW)
    if paired:
        send_select = links.copy(r.select_low, r.far_select, mate)
        send_select.start()
    else:
        big_grad(r.part_select, r.select_low, r.normed[...], state)
        select_streams = [stream_start(bufs_select, 0)]
    stream_b(gate_streams[0])
    stream_c(out_streams[2])

    if paired:
        pair_grad(r.part_value, r.gate, r.far_value, send_value, value_streams)
        send_select.wait()
        total = product(r.select_low[...], r.normed[:, own_half], 0, 0)
        total = total + product(r.far_select[...], r.far_normed[...], 0, 0)
        r.part_select[0] = total.astype(LOW)
        stream_up(select_streams[0])
        for copy in send_hidden:
            copy.wait_send()
    else:
        for me in value_streams + select_streams:
            stream_a(me)
    stream_b(gate_streams[1])
    stream_c(gate_streams[0])

    branch_last.wait()

    def output_rows(i, _):
        at = block(i * 64, 64)
        total = (
            r.branch[h, at, :].astype(WIDE)
            + r.branch_near[0, at, :].astype(WIDE)
            + r.branch_far[at, :].astype(WIDE)
        )
        r.o_block[at, :] = (r.x_all[h, at, :].astype(WIDE) + total).astype(LOW)
        return 0

    lax.fori_loop(0, total_rows // 64, output_rows, 0)
    for k in range(head_count):
        columns = slice(k * piece, (k + 1) * piece)

        def d_normed_rows(q, _):
            at = block(q * rows, rows)
            total = product(r.gate_low[at, :], r.v_w_gate[columns, :], 1, 1)
            total = total + product(r.gate[at, :], r.v_w_value[columns, :], 1, 1)
            total = total + product(r.select_low[at, :], r.v_w_select[:, columns])
            mean = jnp.sum(
                total * r.x_all[k, at, :].astype(WIDE) * r.gain_all[k, 0:1, :],
                axis=1,
                keepdims=True,
            )
            r.branch[k, at, :] = total.astype(LOW)
            if k == 0:
                r.sums[at, :] = jnp.where(iota((rows, state), 1) == 0, mean, 0.0)
            else:
                r.sums[at, :] += jnp.where(iota((rows, state), 1) == 0, mean, 0.0)
            return 0

        lax.fori_loop(0, seqs, d_normed_rows, 0)
    normed_copies = spread_parts(r.branch, r.normed_near)
    mean_copies = row_sums(r.mean_own, r.mean_held)
    stream_b(gate_streams[2])
    stream_c(gate_streams[1])
    stream_b(value_streams[0])
    normed_last = spread_over(r.branch, r.normed_near, r.sent, r.normed_far, normed_copies)
    row_sums_end(r.mean_own, r.mean_held, mean_copies)
    normed_last.wait()

    def input_rows(i, total):
        at = block(i * 32, 32)
        grad = (
            r.branch[h, at, :].astype(WIDE)
            + r.normed_near[0, at, :].astype(WIDE)
            + r.normed_far[at, :].astype(WIDE)
        )
        own = r.x_all[h, at, :].astype(WIDE)
        inverse = r.inverse[at, 0:1]
        mean = r.sums[at, 0:1] / model
        r.o_input[at, :] = (
            r.cot_all[h, at, :].astype(WIDE)
            + inverse * (grad * r.gain_all[h, 0:1, :])
            - own * (inverse * inverse * inverse * mean)
        )
        term = grad * own * inverse
        for t in range(4):
            total = total + term[t * 8 : t * 8 + 8]
        return total

    gain_grad = lax.fori_loop(0, total_rows // 32, input_rows, jnp.zeros((8, piece), WIDE))
    small[7:8, 0:piece] = jnp.sum(gain_grad, axis=0, keepdims=True)

    small_copies = []
    for j in range(1, seq_count):
        copy = links.copy(small, r.small_seq.at[j - 1], {SEQ: lax.rem(s + j, seq_count)})
        copy.start()
        small_copies.append(copy)
    stream_c(gate_streams[2])
    stream_b(value_streams[1])
    stream_c(value_streams[0])
    stream_b(value_streams[2])
    stream_c(value_streams[1])
    stream_b(select_streams[0])
    stream_c(value_streams[2])
    stream_c(select_streams[0])
    total = small[...]
    for j, copy in enumerate(small_copies):
        copy.wait()
    for j in range(seq_count - 1):
        total = total + r.small_seq[j]
    r.small_mid[...] = total
    small_copies = []
    for j in range(1, dp_count):
        copy = links.copy(r.small_mid, r.small_dp.at[j - 1], {DP: lax.rem(d + j, dp_count)})
        copy.start()
        small_copies.append(copy)
    for copy in small_copies:
        copy.wait()
    for j in range(dp_count - 1):
        total = total + r.small_dp[j]
    r.o_small[:, 0:inner] = total[:, 0:inner]
    taps_grad, by_head = total[:, inner : inner + state], total[:, inner + state :]
    r.o_small[:, inner : inner + state] = jnp.where(odd, pltpu.roll(taps_grad, half, 1), taps_grad)
    r.o_small[:, inner + state :] = jnp.where(odd, by_head, pltpu.roll(by_head, half, 1))
    for me in keeps:
        stream_d(me)

    @pl.when(s > 0)
    def _():
        for copy in rim_back + rim_back_s:
            copy.wait_send()
        for c in range(chunk_total):
            hop_copy(r.adj_in, r.adj_out, backward_first, c, False)[1].wait_send()

    assert links.count <= size.links, links.count


def finish_kernel(half, heads, piece, inner, *refs):
    ins, outs = refs[:7], refs[7:]
    for source, target in zip(ins[:5], outs[:5]):
        target[...] = source[...].astype(target.dtype)
    matrix, small = ins[5:]
    g_select, g_step, g_norm, g_conv, g_bias, g_conv_s, g_bias_s, g_bias_h, g_decay, g_skip, g_gain = outs[5:]

    @pl.when(pl.program_id(0) == 0)
    def _():
        odd = lax.rem(lax.axis_index(HEAD), 2) == 1
        low_rows, high_rows = matrix[0:half, :].astype(WIDE), matrix[half : 2 * half, :].astype(WIDE)
        g_select[...] = jnp.where(odd, high_rows, low_rows)
        g_step[...] = jnp.where(odd, low_rows, high_rows)[0:heads, :]
        g_norm[...] = small[7, 0:piece]
        g_conv[...] = small[0:4, 0:inner]
        g_bias[...] = small[4, 0:inner]
        g_gain[...] = small[5, 0:inner]
        g_conv_s[...] = small[0:4, inner : inner + half]
        g_bias_s[...] = small[4, inner : inner + half]
        for row, target in enumerate((g_bias_h, g_decay, g_skip)):
            target[...] = small[row, inner + 2 * half : inner + 2 * half + heads]


def body(size, *args):
    (
        block_input,
        norm_gain,
        w_gate,
        w_value,
        w_select,
        w_step,
        conv_value,
        bias_value,
        conv_select,
        bias_select,
        step_bias,
        decay_log,
        skip_gain,
        gate_gain,
        w_out,
        out_cotangent,
    ) = args
    seqs, rows, piece = block_input.shape
    heads, inner = skip_gain.shape[0], w_value.shape[1]
    head_axis, seq_axis, dp_axis = size[HEAD], size[SEQ], size[DP]
    half = w_select.shape[1]
    state = half * head_axis // 2
    width = inner // heads
    model = piece * head_axis
    total_rows = seqs * rows
    assert head_axis == 4 and seq_axis == 4 and 2 * half == state and heads <= half and 2 * width == state

    vmem = pl.BlockSpec(memory_space=pltpu.VMEM)
    anywhere = pl.BlockSpec(memory_space=pl.ANY)
    inputs = dict(
        x=(block_input.reshape(total_rows, piece), anywhere),
        cot=(out_cotangent.reshape(total_rows, piece), anywhere),
        bias_value=(bias_value, vmem),
        gate_gain=(gate_gain, vmem),
        norm_gain=(norm_gain, vmem),
        bias_select=(bias_select, vmem),
        step_bias=(step_bias, vmem),
        decay_log=(decay_log, vmem),
        skip_gain=(skip_gain, vmem),
        conv_value=(conv_value, vmem),
        conv_select=(conv_select, vmem),
        w_select=(w_select.T, vmem),
        w_step=(w_step.T, vmem),
        w_value=(w_value, anywhere),
        w_gate=(w_gate, anywhere),
        w_out=(w_out, anywhere),
    )
    small_shape = (8, inner + 2 * state)

    def result(shape, kind, spec):
        return (jax.ShapeDtypeStruct(shape, kind), spec)

    outputs = dict(
        o_block=result((total_rows, piece), LOW, vmem),
        o_input=result((total_rows, piece), WIDE, vmem),
        o_small=result(small_shape, WIDE, vmem),
        out_out=result((inner, model), LOW, anywhere),
        out_gate=result((model, inner), LOW, anywhere),
        out_value=result((model, inner), LOW, anywhere),
        out_select=result((state, model), LOW, anywhere),
    )
    link_total = 128 + 16 * dp_axis

    def wide(*shape):
        return pltpu.VMEM(shape, WIDE)

    def low(*shape):
        return pltpu.VMEM(shape, LOW)

    def wide_tokens(lanes, extra=0):
        return wide(seqs, rows + extra, lanes)

    def low_tokens(lanes):
        return low(seqs, rows, lanes)

    def over_of(chunks, depth, columns):
        return low(chunks, dp_axis - 1, depth // (chunks * dp_axis), columns)

    def cut_of(chunks, depth, columns):
        return low(chunks, depth // (chunks * dp_axis), columns)

    semaphores = pltpu.SemaphoreType.DMA
    scratch = dict(
        send_sem=semaphores((link_total,)),
        recv_sem=semaphores((link_total,)),
        load_sem=semaphores((5,)),
        keep_sem=semaphores((10,)),
        v_w_select=low(state, model),
        v_w_value=low(model, inner),
        v_w_gate=low(model, inner),
        v_w_out=low(inner, model),
        gain_all=wide(head_axis, 8, piece),
        x_all=low(head_axis, total_rows, piece),
        cot_all=low(head_axis, total_rows, piece),
        normed=low(total_rows, model),
        inverse=wide(total_rows, state),
        expand=low(state, inner),
        tri=low(rows, rows),
        taps=wide(8, state),
        step_arg=wide_tokens(state),
        step=wide_tokens(state),
        running=wide_tokens(state),
        row_part=wide_tokens(state),
        step_grad=wide_tokens(state),
        sel_keep=wide_tokens(state),
        running_t=wide(seqs, state, rows),
        col_part=wide(seqs, state, rows),
        running_x=wide_tokens(heads * state),
        step_x=wide_tokens(inner),
        scale_x=wide_tokens(inner),
        mixed=wide_tokens(inner),
        inter=wide_tokens(inner),
        projected=wide_tokens(inner),
        act=low_tokens(inner),
        weighted=low_tokens(inner),
        weighted_tail=low_tokens(inner),
        d_mixed_low=low_tokens(inner),
        d_growth=low_tokens(inner),
        value_ext=wide_tokens(inner, RIM),
        select_ext=wide_tokens(state, RIM),
        slope_v=wide_tokens(inner, RIM),
        slope_s=wide_tokens(state, RIM),
        select_own=low_tokens(state),
        select_side=low_tokens(state),
        select_pair=low_tokens(state),
        select_over=low_tokens(state),
        b_all=low_tokens(state),
        c_all=low_tokens(state),
        sel_send=low_tokens(state),
        sel_over=low_tokens(state),
        sel_pair=low_tokens(state),
        sel_side=low_tokens(state),
        gram=wide(seqs, rows, rows),
        pair_weight=wide(seqs, rows, rows),
        state_local=wide(seqs, inner, state),
        decay_row=wide(seqs, inner, state),
        state_in=low(seqs, inner, state),
        state_out=low(seqs, inner, state),
        adj_in=low(seqs, inner, state),
        adj_out=low(seqs, inner, state),
        gate=low(total_rows, inner),
        hidden=low(total_rows, inner),
        gate_low=low(total_rows, inner),
        select_low=low(total_rows, state),
        skip_x=wide(8, inner),
        sums=wide(total_rows, state),
        sum_own=wide(8, total_rows),
        sum_held=wide(head_axis - 1, 8, total_rows),
        mean_own=wide(8, total_rows),
        mean_held=wide(head_axis - 1, 8, total_rows),
        branch=low(head_axis, total_rows, piece),
        sent=low(total_rows, piece),
        branch_near=low(2, total_rows, piece),
        branch_far=low(total_rows, piece),
        normed_near=low(2, total_rows, piece),
        normed_far=low(total_rows, piece),
        small=wide(*small_shape),
        small_mid=wide(*small_shape),
        small_seq=wide(seq_axis - 1, *small_shape),
        small_dp=wide(dp_axis - 1, *small_shape),
    )
    if dp_axis == 2:
        scratch.update(
            far_normed=low(total_rows, model // 2),
            far_cot=low(head_axis // 2, total_rows, piece),
            far_hidden=low(3, total_rows, inner // 3),
            far_gate=low(3, total_rows, inner // 3),
            far_value=low(3, total_rows, inner // 3),
            far_select=low(total_rows, state),
            part_out=low(3, inner // 3, model // 2),
            part_gate=low(3, model // 2, inner // 3),
            part_value=low(3, model // 2, inner // 3),
            part_select=low(1, state, model // 2),
            up_out=low(3, inner // 3, model // 2),
            mid_out=low(3, inner // 3, model // 2),
            up_gate=low(3, model // 2, inner // 3),
            mid_gate=low(3, model // 2, inner // 3),
            up_value=low(3, model // 2, inner // 3),
            mid_value=low(3, model // 2, inner // 3),
            up_select=low(1, state, model // 2),
            mid_select=low(1, state, model // 2),
        )
    else:
        scratch.update(
            part_out=low(inner, model),
            part_gate=low(model, inner),
            part_value=low(model, inner),
            part_select=low(state, model),
            over_out=over_of(3, inner, model),
            over_gate=over_of(3, model, inner),
            over_value=over_of(3, model, inner),
            over_select=over_of(1, state, model),
            up_out=cut_of(3, inner, model),
            up_gate=cut_of(3, model, inner),
            up_value=cut_of(3, model, inner),
            up_select=cut_of(1, state, model),
            mid_out=cut_of(3, inner, model),
            mid_gate=cut_of(3, model, inner),
            mid_value=cut_of(3, model, inner),
            mid_select=cut_of(1, state, model),
        )
    facts = SimpleNamespace(
        names=list(inputs) + list(outputs) + list(scratch),
        seqs=seqs,
        rows=rows,
        heads=heads,
        width=width,
        inner=inner,
        state=state,
        piece=piece,
        head_axis=head_axis,
        seq_axis=seq_axis,
        dp_axis=dp_axis,
        links=link_total,
    )
    results = pl.pallas_call(
        functools.partial(mixer_kernel, facts),
        out_shape=[shape for shape, _ in outputs.values()],
        in_specs=[spec for _, spec in inputs.values()],
        out_specs=[spec for _, spec in outputs.values()],
        scratch_shapes=list(scratch.values()),
        compiler_params=pltpu.CompilerParams(
            collective_id=0, has_side_effects=True, vmem_limit_bytes=67043328
        ),
    )(*[value for value, _ in inputs.values()])
    got = SimpleNamespace(**dict(zip(outputs, results, strict=True)))
    steps = 4

    def by_rows(depth, columns):
        return pl.BlockSpec((depth // steps, columns), lambda i: (i, 0))

    def whole(*shape):
        return pl.BlockSpec(shape, lambda i: (0,) * len(shape))

    streamed = [(total_rows, piece), (total_rows, piece), (inner, model), (model, inner), (model, inner)]
    kinds = [LOW, WIDE, WIDE, WIDE, WIDE]
    fixed = [
        (half, model),
        (heads, model),
        (piece,),
        (4, inner),
        (inner,),
        (4, half),
        (half,),
        (heads,),
        (heads,),
        (heads,),
        (inner,),
    ]
    final = pl.pallas_call(
        functools.partial(finish_kernel, half, heads, piece, inner),
        grid=(steps,),
        out_shape=[jax.ShapeDtypeStruct(shape, kind) for shape, kind in zip(streamed, kinds)]
        + [jax.ShapeDtypeStruct(shape, WIDE) for shape in fixed],
        in_specs=[by_rows(*shape) for shape in streamed]
        + [whole(state, model), whole(*small_shape)],
        out_specs=[by_rows(*shape) for shape in streamed] + [whole(*shape) for shape in fixed],
    )(
        got.o_block,
        got.o_input,
        got.out_out,
        got.out_gate,
        got.out_value,
        got.out_select,
        got.o_small,
    )
    block_output, input_grad, g_out, g_gate, g_value, g_select, g_step = final[:7]
    g_norm, g_conv, g_bias, g_conv_s, g_bias_s, g_step_bias, g_decay, g_skip, g_gain = final[7:]
    return (
        block_output.reshape(seqs, rows, piece),
        input_grad.reshape(seqs, rows, piece),
        g_norm,
        g_gate,
        g_value,
        g_select.T,
        g_step.T,
        g_conv,
        g_bias,
        g_conv_s,
        g_bias_s,
        g_step_bias,
        g_decay,
        g_skip,
        g_gain,
        g_out,
    )


def solution(mesh):
    columns, single, tokens = P(None, HEAD), P(HEAD), P(DP, SEQ, HEAD)
    in_specs = (
        tokens,
        single,
        columns,
        columns,
        columns,
        columns,
        columns,
        single,
        columns,
        single,
        single,
        single,
        single,
        single,
        P(HEAD, None),
        tokens,
    )
    out_specs = (
        tokens,
        tokens,
        single,
        columns,
        columns,
        columns,
        columns,
        columns,
        single,
        columns,
        single,
        single,
        single,
        single,
        single,
        P(HEAD, None),
    )
    return jax.shard_map(
        functools.partial(body, dict(mesh.shape)),
        mesh=mesh,
        in_specs=in_specs,
        out_specs=out_specs,
        check_vma=False,
    )
```

```python
import functools
from types import SimpleNamespace

import jax
import jax.numpy as jnp
from jax import lax
from jax.experimental import pallas as pl
from jax.experimental.pallas import tpu as pltpu
from jax.sharding import PartitionSpec as P

EPSILON = 1e-05
LOW = jnp.bfloat16
WIDE = jnp.float32
MESH = pl.DeviceIdType.MESH
RIM = 8
NEVER = -1e30
HEAD, SEQ, DP = "head", "seq", "dp"


def product(left, right, left_dim=1, right_dim=0):
    return lax.dot_general(
        left,
        right,
        (((left_dim,), (right_dim,)), ((), ())),
        preferred_element_type=WIDE,
    )


def pieces_of(values, count):
    found = []
    for _ in range(count):
        low = values.astype(LOW)
        found.append(low)
        values = values - low.astype(WIDE)
    return found


def picked(left, table, left_dim=1, table_dim=0, count=3):
    parts = [product(part, table, left_dim, table_dim) for part in pieces_of(left, count)]
    return functools.reduce(jnp.add, parts[::-1])


def picked_by(table, right, table_dim=1, right_dim=0, count=3):
    parts = [product(table, part, table_dim, right_dim) for part in pieces_of(right, count)]
    return functools.reduce(jnp.add, parts[::-1])


def iota(shape, dim):
    return lax.broadcasted_iota(jnp.int32, shape, dim)


def sigmoid(values):
    return 1.0 / (1.0 + jnp.exp(-values))


def softplus(values):
    return jnp.maximum(values, 0.0) + jnp.log1p(jnp.exp(-jnp.abs(values)))


def block(start, size):
    return pl.ds(pl.multiple_of(start, size), size)


class Links:
    def __init__(self, send_sem, recv_sem):
        self.send_sem, self.recv_sem, self.count = send_sem, recv_sem, 0

    def reserve(self, number):
        first = self.count
        self.count += number
        return first

    def copy(self, source, target, where, slot=None):
        slot = self.reserve(1) if slot is None else slot
        return pltpu.make_async_remote_copy(
            src_ref=source,
            dst_ref=target,
            send_sem=self.send_sem.at[slot],
            recv_sem=self.recv_sem.at[slot],
            device_id=where,
            device_id_type=MESH,
        )


def mixer_kernel(size, *refs):
    r = SimpleNamespace(**dict(zip(size.names, refs, strict=True)))
    seqs, rows, heads, width = size.seqs, size.rows, size.heads, size.width
    inner, state, piece = size.inner, size.state, size.piece
    head_count, seq_count, dp_count = size.head_axis, size.seq_axis, size.dp_axis
    inner_total, model = inner * head_count, piece * head_count
    total_rows = seqs * rows
    half = state // 2
    links = Links(r.send_sem, r.recv_sem)
    h, s, d = lax.axis_index(HEAD), lax.axis_index(SEQ), lax.axis_index(DP)
    side, over, across = h ^ 1, h ^ 2, h ^ 3
    place = lax.rem(h, 2) * half
    spare = half - place

    loads = []
    weights = (
        (r.w_value, r.v_w_value),
        (r.w_gate, r.v_w_gate),
        (r.w_out, r.v_w_out),
    )
    for index, (source, target) in enumerate(weights):
        load = pltpu.make_async_copy(source, target, r.load_sem.at[index])
        load.start()
        loads.append(load)

    barrier = pltpu.get_barrier_semaphore()
    peers = [{HEAD: lax.rem(h + j, head_count)} for j in range(1, head_count)]
    peers += [{SEQ: lax.rem(s + j, seq_count)} for j in range(1, seq_count)]
    peers += [{DP: lax.rem(d + j, dp_count)} for j in range(1, dp_count)]
    for peer in peers:
        pl.semaphore_signal(barrier, inc=1, device_id=peer, device_id_type=MESH)
    pl.semaphore_wait(barrier, len(peers))

    def gather_start(own, held):
        near = links.copy(own, held.at[h], {HEAD: side})
        far = links.copy(own, held.at[h], {HEAD: over})
        far.start()
        near.start()
        return (near, far)

    def gather_pass(held, pair):
        pair[1].wait_recv()
        forward = links.copy(held.at[over], held.at[over], {HEAD: side})
        forward.start()
        return pair + (forward,)

    def gather_end(copies):
        copies[0].wait_recv()
        copies[2].wait_recv()
        for copy in copies:
            copy.wait_send()

    r.gain_all[h] = jnp.broadcast_to(r.norm_gain[...][None].astype(WIDE), (8, piece))
    gain_copies = gather_start(r.gain_all.at[h], r.gain_all)
    input_copies = gather_start(r.x, r.x_all)
    cot_copies = gather_start(r.cot, r.cot_all)

    own_x = pltpu.make_async_copy(r.x, r.x_all.at[h], r.load_sem.at[3])
    own_cot = pltpu.make_async_copy(r.cot, r.cot_all.at[h], r.load_sem.at[4])
    own_x.start()
    own_cot.start()

    odd = lax.rem(h, 2) == 1
    r.expand[...] = jnp.where(
        (iota((state, inner), 1) // width + spare) == iota((state, inner), 0), 1.0, 0.0
    ).astype(LOW)
    lower = iota((rows, rows), 0) >= iota((rows, rows), 1)
    r.tri[...] = jnp.where(lower, 1.0, 0.0).astype(LOW)
    shift = jnp.where(iota((half, state), 0) + place == iota((half, state), 1), 1.0, 0.0).astype(LOW)
    r.taps[0:4, :] = picked(r.conv_select[...], shift)
    few = jnp.broadcast_to(r.bias_select[...][None], (8, half))
    r.taps[4:5, :] = picked(few, shift)[0:1, :]
    moved = jnp.where(
        iota((heads, state), 0) + spare == iota((heads, state), 1), 1.0, 0.0
    ).astype(LOW)
    for row, source in enumerate((r.step_bias, r.decay_log, r.skip_gain)):
        few = jnp.broadcast_to(source[...][None], (8, heads))
        r.taps[5 + row : 6 + row, :] = picked(few, moved)[0:1, :]
    r.v_w_select[...] = jnp.zeros((state, model), LOW)
    r.v_w_select[pl.ds(pl.multiple_of(place, half), half), :] = r.w_select[...]
    padded = jnp.concatenate([r.w_step[...], jnp.zeros((16 - heads, model), LOW)], axis=0)
    r.v_w_select[pl.ds(pl.multiple_of(spare, half), 16), :] = padded

    @pl.when(s == 0)
    def _():
        r.value_ext[:, 0:RIM, :] = jnp.zeros((seqs, RIM, inner), WIDE)
        r.select_ext[:, 0:RIM, :] = jnp.zeros((seqs, RIM, state), WIDE)
        r.state_in[...] = jnp.zeros((seqs, inner, state), LOW)

    @pl.when(s == seq_count - 1)
    def _():
        r.slope_v[:, rows : rows + RIM, :] = jnp.zeros((seqs, RIM, inner), WIDE)
        r.slope_s[:, rows : rows + RIM, :] = jnp.zeros((seqs, RIM, state), WIDE)
        r.adj_in[...] = jnp.zeros((seqs, inner, state), LOW)

    gain_copies = gather_pass(r.gain_all, gain_copies)
    input_copies = gather_pass(r.x_all, input_copies)
    gather_end(gain_copies)
    gather_end(input_copies)
    own_x.wait()

    def norm_rows(i, _):
        at = block(i * 64, 64)
        total = jnp.zeros((64, 1), WIDE)
        for k in range(head_count):
            part = r.x_all[k, at, :].astype(WIDE)
            total = total + jnp.sum(part * part, axis=1, keepdims=True)
        inverse = lax.rsqrt(total / model + EPSILON)
        r.inverse[at, :] = jnp.broadcast_to(inverse, (64, state))
        for k in range(head_count):
            part = r.x_all[k, at, :].astype(WIDE)
            r.normed[at, k * piece : (k + 1) * piece] = (
                part * inverse * r.gain_all[k, 0:1, :]
            ).astype(LOW)
        return 0

    lax.fori_loop(0, total_rows // 64, norm_rows, 0)

    paired = dp_count == 2
    mate = {DP: lax.rem(d + 1, dp_count)}
    wide_half = model // 2
    own_half = pl.ds(pl.multiple_of(lax.rem(d, 2) * wide_half, 128), wide_half)
    mate_half = pl.ds(pl.multiple_of(lax.rem(d + 1, 2) * wide_half, 128), wide_half)
    halves = head_count // 2

    def chunk_sends(source, target):
        chunks, _, lanes = target.shape
        copies = []
        for c in range(chunks):
            at = slice(c * lanes, (c + 1) * lanes)
            copies.append(links.copy(source.at[:, at], target.at[c], mate))
            copies[-1].start()
        return copies

    if paired:
        send_normed = links.copy(r.normed.at[:, mate_half], r.far_normed, mate)
        send_normed.start()

    for q in range(seqs):
        at = pl.ds(q * rows, rows)
        both = product(r.normed[at, :], r.v_w_select[...], 1, 1)
        r.step_arg[q] = both + r.taps[5:6, :]
        r.select_ext[q, RIM : RIM + rows, :] = both.astype(LOW).astype(WIDE)
    loads[0].wait()

    def value_matmul(q, _):
        at = block(q * rows, rows)
        r.value_ext[q, RIM : RIM + rows, :] = (
            product(r.normed[at, :], r.v_w_value[...]).astype(LOW).astype(WIDE)
        )
        return 0

    lax.fori_loop(0, seqs, value_matmul, 0)
    rims = []
    for ext in (r.select_ext, r.value_ext):
        for q in range(seqs):
            rims.append(
                links.copy(
                    ext.at[q, rows : rows + RIM, :],
                    ext.at[q, 0:RIM, :],
                    {SEQ: lax.rem(s + 1, seq_count)},
                )
            )

    @pl.when(s < seq_count - 1)
    def _():
        for copy in rims:
            copy.start()

    cot_copies = gather_pass(r.cot_all, cot_copies)

    tri = r.tri
    for q in range(seqs):
        step = softplus(r.step_arg[q])
        r.step[q] = step
        rate = -jnp.exp(r.taps[6:7, :])
        fall = step * rate
        running = picked_by(tri[...], fall)
        r.running[q] = running
        r.running_t[q] = picked(fall, tri[...], 0, 1)

        def spread(g, _):
            lanes = 4 * state
            pick = jnp.where(
                iota((state, lanes), 0) == spare + 4 * g + iota((state, lanes), 1) // state, 1.0, 0.0
            ).astype(LOW)
            r.running_x[q, :, block(g * lanes, lanes)] = picked(r.running[q], pick)
            return 0

        lax.fori_loop(0, heads // 4, spread, 0)
        r.step_x[q] = picked(step, r.expand[...], count=2)
        last = running[rows - 1 : rows, :]
        r.scale_x[q] = picked(jnp.exp(last - running), r.expand[...], count=2)
        decay = jnp.broadcast_to(jnp.exp(r.running_t[q, :, rows - 1 : rows]), (state, state))
        r.decay_row[q] = picked_by(r.expand[...], decay, 0, 0, count=2)

    @pl.when(s > 0)
    def _():
        for copy in rims:
            copy.wait_recv()

    @pl.when(s < seq_count - 1)
    def _():
        for copy in rims:
            copy.wait_send()

    lane_row = iota((1, state), 1)
    mine = (lane_row >= place) & (lane_row < place + half)

    def convolve(ext, q, base, count, taps, bias):
        wide = ext[q, pl.ds(pl.multiple_of(base, 8), count + RIM), :]
        total = bias
        for k in range(4):
            total = total + taps[k : k + 1, :] * wide[RIM - 3 + k : RIM - 3 + k + count]
        return total

    value_bias, gate_gain = r.bias_value[...][None], r.gate_gain[...][None]

    for q in range(seqs):
        conv = convolve(r.select_ext, q, 0, rows, r.taps, r.taps[4:5, :])
        act = jnp.where(mine, conv * sigmoid(conv), 0.0)
        r.select_own[q] = act.astype(LOW)
    pair = links.copy(r.select_own, r.select_side, {HEAD: side})
    pair.start()

    def value_conv(i, _):
        q, base = i // (rows // 64), lax.rem(i, rows // 64) * 64
        conv = convolve(r.value_ext, q, base, 64, r.conv_value, value_bias)
        act = (conv * sigmoid(conv)).astype(LOW)
        at = block(base, 64)
        r.act[q, at, :] = act
        r.weighted[q, at, :] = (act.astype(WIDE) * r.step_x[q, at, :]).astype(LOW)
        return 0

    lax.fori_loop(0, seqs * (rows // 64), value_conv, 0)
    pair.wait()
    r.select_pair[...] = r.select_own[...] + r.select_side[...]
    swap = links.copy(r.select_pair, r.select_over, {HEAD: over})
    swap.start()
    loads[1].wait()

    def gate_matmul(q, _):
        at = block(q * rows, rows)
        r.gate[at, :] = product(r.normed[at, :], r.v_w_gate[...]).astype(LOW)
        return 0

    lax.fori_loop(0, seqs, gate_matmul, 0)
    swap.wait()
    gather_end(cot_copies)
    own_cot.wait()
    if paired:
        at = pl.ds(lax.rem(d + 1, 2) * halves, halves)
        send_cot = links.copy(r.cot_all.at[at], r.far_cot, mate)
        send_cot.start()
    upper = h >= 2
    first, second = r.select_pair[...], r.select_over[...]
    r.b_all[...] = jnp.where(upper, second, first)
    r.c_all[...] = jnp.where(upper, first, second)

    for q in range(seqs):
        b = r.b_all[q]
        tailed = (r.weighted[q].astype(WIDE) * r.scale_x[q]).astype(LOW)
        r.weighted_tail[q] = tailed
        r.state_local[q] = product(tailed, b, 0, 0)
        r.gram[q] = product(r.c_all[q], b, 1, 1)
        r.scale_x[q] = picked(jnp.exp(r.running[q]), r.expand[...], count=2)

    chunk_rows = inner // 3

    chunk_total = 3 * seqs

    def hop_copy(held, sent, first, c, forward):
        at = pl.ds(pl.multiple_of(lax.rem(c, 3) * chunk_rows, 16), chunk_rows)
        to = lax.rem(s + (1 if forward else seq_count - 1), seq_count)
        return at, links.copy(sent.at[c // 3, at, :], held.at[c // 3, at, :], {SEQ: to}, first + c)

    def hop(held, local, sent, first, c, forward):
        q = c // 3
        at, copy = hop_copy(held, sent, first, c, forward)

        @pl.when((s > 0) if forward else (s < seq_count - 1))
        def _():
            copy.wait_recv()

        sent[q, at, :] = (
            local[q, at, :] + r.decay_row[q, at, :] * held[q, at, :].astype(WIDE)
        ).astype(LOW)

        @pl.when((s < seq_count - 1) if forward else (s > 0))
        def _():
            copy.start()

    half_lane = iota((rows, state), 1) < width

    def decay_of(q, g):
        column = r.running_x[q, :, block(g * state, state)]
        gap = jnp.concatenate([column] * (rows // state), axis=1) - r.running_t[q, pl.ds(spare + g, 1), :]
        return jnp.exp(jnp.where(lower, gap, NEVER))

    def forward_pair(i, _):
        q, j = i // (heads // 2), lax.rem(i, heads // 2)
        at = block(j * state, state)
        values = r.weighted[q, :, at]
        zero = jnp.zeros_like(values)
        total = jnp.zeros((rows, state), WIDE)
        for part in range(2):
            mixing = (r.gram[q] * decay_of(q, 2 * j + part)).astype(LOW)
            kept = jnp.where(half_lane if part == 0 else ~half_lane, values, zero)
            total = total + product(mixing, kept)
        r.mixed[q, :, at] = total
        return 0

    pair_total = seqs * heads // 2
    forward_first = links.reserve(chunk_total)

    def forward_slot(i, _):
        @pl.when(i < pair_total)
        def _():
            forward_pair(i, 0)

        c = i - chunk_total * s

        @pl.when((c >= 0) & (c < chunk_total))
        def _():
            hop(r.state_in, r.state_local, r.state_out, forward_first, c, True)

        return 0

    lax.fori_loop(0, pair_total, forward_slot, 0)
    loads[2].wait()

    def d_hidden_matmul(q, _):
        at = block(q * rows, rows)
        total = product(r.cot_all[0, at, :], r.v_w_out[:, 0:piece], 1, 1)
        for k in range(1, head_count):
            total = total + product(
                r.cot_all[k, at, :], r.v_w_out[:, k * piece : (k + 1) * piece], 1, 1
            )
        r.projected[q] = total
        return 0

    lax.fori_loop(0, seqs, d_hidden_matmul, 0)
    lax.fori_loop(pair_total, max(pair_total, chunk_total * seq_count), forward_slot, 0)

    r.skip_x[...] = picked(jnp.broadcast_to(r.taps[7:8, :], (8, state)), r.expand[...])
    for q in range(seqs):
        r.inter[q] = product(r.c_all[q], r.state_in[q], 1, 1) * r.scale_x[q]

    tile = 32
    lanes_tile = iota((tile, state), 1)

    def gate_rows(i, _):
        q, base = i // (rows // tile), lax.rem(i, rows // tile) * tile
        at, flat = block(base, tile), block(i * tile, tile)
        mixed = (
            r.mixed[q, at, :]
            + r.inter[q, at, :]
            + r.skip_x[0:1, :] * r.act[q, at, :].astype(WIDE)
        )
        r.mixed[q, at, :] = mixed
        gate = r.gate[flat, :].astype(WIDE)
        gated = mixed * (gate * sigmoid(gate))
        squares = jnp.sum(gated * gated, axis=1, keepdims=True)
        dots = jnp.sum(gated * r.projected[q, at, :] * gate_gain, axis=1, keepdims=True)
        r.sums[flat, :] = jnp.where(lanes_tile == 0, squares, jnp.where(lanes_tile == 1, dots, 0.0))
        return 0

    lax.fori_loop(0, total_rows // tile, gate_rows, 0)
    picks = jnp.where(iota((8, state), 0) == iota((8, state), 1), 1.0, 0.0).astype(LOW)

    def row_sums(own, held):
        own[...] = picked_by(picks, r.sums[...], 1, 1)
        copies = []
        for j in range(1, head_count):
            copy = links.copy(own, held.at[j - 1], {HEAD: h ^ j})
            copy.start()
            copies.append(copy)
        return copies

    def row_sums_end(own, held, copies):
        total = own[...]
        for j, copy in enumerate(copies):
            copy.wait_recv()
            total = total + held[j]
        r.sums[...] = picked(total, picks, 0, 0)
        for copy in copies:
            copy.wait_send()

    sum_copies = row_sums(r.sum_own, r.sum_held)

    @pl.when(s < seq_count - 1)
    def _():
        for c in range(chunk_total):
            hop_copy(r.state_in, r.state_out, forward_first, c, True)[1].wait_send()

    row_sums_end(r.sum_own, r.sum_held, sum_copies)

    small = r.small
    small[...] = jnp.zeros(small.shape, WIDE)

    def norm_back(i, carry):
        gain_total, skip_total = carry
        q, base = i // (rows // tile), lax.rem(i, rows // tile) * tile
        at, flat = block(base, tile), block(i * tile, tile)
        sums = r.sums[flat, :]
        scale = lax.rsqrt(sums[:, 0:1] / inner_total + EPSILON)
        mean = scale * scale * scale * (sums[:, 1:2] / inner_total)
        mixed = r.mixed[q, at, :]
        gate = r.gate[flat, :].astype(WIDE)
        logistic = sigmoid(gate)
        gate_act = gate * logistic
        gated = mixed * gate_act
        normal = gated * scale
        grad = r.projected[q, at, :]
        gain = gate_gain
        r.hidden[flat, :] = (normal * gain).astype(LOW)
        d_gated = scale * (grad * gain) - gated * mean
        d_mixed = d_gated * gate_act
        r.d_mixed_low[q, at, :] = d_mixed.astype(LOW)
        r.d_growth[q, at, :] = (d_mixed * r.scale_x[q, at, :]).astype(LOW)
        r.gate_low[flat, :] = (
            d_gated * mixed * (logistic * (1.0 + gate * (1.0 - logistic)))
        ).astype(LOW)
        gain_part = grad * normal
        skip_part = d_mixed * r.act[q, at, :].astype(WIDE)
        for k in range(tile // 8):
            gain_total = gain_total + gain_part[k * 8 : k * 8 + 8]
            skip_total = skip_total + skip_part[k * 8 : k * 8 + 8]
        return gain_total, skip_total

    blank = jnp.zeros((8, inner), WIDE)
    gain_total, skip_total = lax.fori_loop(0, total_rows // tile, norm_back, (blank, blank))
    small[5:6, 0:inner] = jnp.sum(gain_total, axis=0, keepdims=True)
    lanes = slice(inner + state, inner + 2 * state)
    skip_total = jnp.broadcast_to(jnp.sum(skip_total, axis=0, keepdims=True), (8, inner))
    small[2:3, lanes] = picked(skip_total, r.expand[...], 1, 1)[0:1, :]

    if paired:
        send_hidden = chunk_sends(r.hidden, r.far_hidden)
        send_gate = chunk_sends(r.gate_low, r.far_gate)

    for q in range(seqs):
        r.state_local[q] = product(r.d_growth[q], r.c_all[q], 0, 0)

    ends = (s == 0) | (s == seq_count - 1)
    inside = (s > 0) & (s < seq_count - 1)

    keeps = []

    def stream_links(own, up, mid, target):
        me = SimpleNamespace(own=own, up=up, mid=mid, copies=[])
        me.copy_up = links.copy(own, up, {SEQ: s ^ 1})
        me.copy_mid = links.copy(own, mid, {SEQ: seq_count - 1 - s})
        me.copy_down = links.copy(up, up, {SEQ: s ^ 1})
        me.keep = pltpu.make_async_copy(up, target, r.keep_sem.at[len(keeps)])
        me.copies_out = [
            links.copy(up, target, {DP: lax.rem(d + j, dp_count)}) for j in range(1, dp_count)
        ]
        keeps.append(me)
        return me

    def stream_start(bufs, chunk):
        part, over, up, mid, out = bufs
        depth = up.shape[1]

        def rows_of(p):
            return pl.ds(pl.multiple_of((chunk * dp_count + p) * depth, 16), depth)

        me = stream_links(part.at[rows_of(d), :], up.at[chunk], mid.at[chunk], out.at[rows_of(d), :])
        me.over = over.at[chunk]
        for j in range(1, dp_count):
            to = lax.rem(d + j, dp_count)
            copy = links.copy(part.at[rows_of(to), :], me.over.at[j - 1], {DP: to})
            copy.start()
            me.copies.append(copy)
        return me

    def pair_streams(part, up, mid, out, by_columns):
        made = []
        for chunk in range(up.shape[0]):
            if by_columns:
                depth = up.shape[1]
                target = out.at[chunk * depth : (chunk + 1) * depth, own_half]
            else:
                lanes = up.shape[2]
                first = pl.multiple_of(lax.rem(d, 2) * wide_half, 16)
                target = out.at[pl.ds(first, wide_half), chunk * lanes : (chunk + 1) * lanes]
            made.append(stream_links(part.at[chunk], up.at[chunk], mid.at[chunk], target))
        return made

    def add_rows(first, target, terms):
        depth = target.shape[0]
        step = next(t for t in (64, 48, 16) if depth % t == 0)

        def add(i, _):
            at = pl.ds(pl.multiple_of(i * step, 16), step)
            total = first[at, :].astype(WIDE)
            for term in terms:
                total = total + term[at, :].astype(WIDE)
            target[at, :] = total.astype(LOW)
            return 0

        lax.fori_loop(0, depth // step, add, 0)

    def stream_up(me):
        @pl.when(ends)
        def _():
            me.copy_up.start()

    def stream_a(me):
        for copy in me.copies:
            copy.wait_recv()
        add_rows(me.own, me.own, [me.over.at[j] for j in range(dp_count - 1)])
        stream_up(me)

    def stream_b(me):
        @pl.when(inside)
        def _():
            me.copy_up.wait_recv()
            add_rows(me.own, me.own, [me.up])
            me.copy_mid.start()

    def stream_c(me):
        @pl.when(inside)
        def _():
            me.copy_mid.wait_recv()
            add_rows(me.own, me.up, [me.mid])
            me.copy_down.start()

        @pl.when(ends)
        def _():
            me.copy_down.wait_recv()

        me.keep.start()
        for copy in me.copies_out:
            copy.start()

    def stream_d(me):
        for copy in me.copies_out:
            copy.wait()
        for copy in me.copies:
            copy.wait_send()
        me.keep.wait()

        @pl.when(ends)
        def _():
            me.copy_up.wait_send()

        @pl.when(inside)
        def _():
            me.copy_mid.wait_send()
            me.copy_down.wait_send()

    def pair_grad(part, right, far_right, sends, made):
        lanes = part.shape[2]
        for c, copy in enumerate(sends):
            copy.wait()
            at = slice(c * lanes, (c + 1) * lanes)
            for start in range(0, wide_half, piece):
                first = lax.rem(d, 2) * wide_half + start
                left = r.normed[:, pl.ds(pl.multiple_of(first, 128), piece)]
                total = product(left, right[:, at], 0, 0)
                total = total + product(r.far_normed[:, start : start + piece], far_right[c], 0, 0)
                part[c, start : start + piece, :] = total.astype(LOW)
            stream_up(made[c])

    def out_grad():
        for c, copy in enumerate(send_hidden):
            copy.wait_recv()
            lanes = r.far_hidden.shape[2]
            for k in range(halves):
                left = r.hidden[:, c * lanes : (c + 1) * lanes]
                total = product(left, r.cot_all[lax.rem(d, 2) * halves + k], 0, 0)
                total = total + product(r.far_hidden[c], r.far_cot[k], 0, 0)
                r.part_out[c, :, k * piece : (k + 1) * piece] = total.astype(LOW)
            stream_up(out_streams[c])

    def big_grad(part, left, right, lanes):
        for start in range(0, part.shape[0], lanes):
            columns = slice(start, start + lanes)
            part[columns, :] = product(left[:, columns], right, 0, 0).astype(LOW)

    if paired:
        out_streams = pair_streams(r.part_out, r.up_out, r.mid_out, r.out_out, True)
        gate_streams = pair_streams(r.part_gate, r.up_gate, r.mid_gate, r.out_gate, False)
        value_streams = pair_streams(r.part_value, r.up_value, r.mid_value, r.out_value, False)
        select_streams = pair_streams(r.part_select, r.up_select, r.mid_select, r.out_select, True)
    else:
        bufs_gate = (r.part_gate, r.over_gate, r.up_gate, r.mid_gate, r.out_gate)
        bufs_out = (r.part_out, r.over_out, r.up_out, r.mid_out, r.out_out)
        bufs_value = (r.part_value, r.over_value, r.up_value, r.mid_value, r.out_value)
        bufs_select = (r.part_select, r.over_select, r.up_select, r.mid_select, r.out_select)
        big_grad(r.part_gate, r.normed, r.gate_low[...], piece)
        gate_streams = [stream_start(bufs_gate, c) for c in range(r.up_gate.shape[0])]

    def spread_parts(part, near):
        copies = [
            links.copy(part.at[side], near.at[0], {HEAD: side}),
            links.copy(part.at[across], near.at[1], {HEAD: side}),
        ]
        for copy in copies:
            copy.start()
        return copies

    def spread_over(part, near, sent, far, copies):
        for copy in copies:
            copy.wait_recv()

        def add(i, _):
            at = block(i * 64, 64)
            sent[at, :] = (
                part[over, at, :].astype(WIDE) + near[1, at, :].astype(WIDE)
            ).astype(LOW)
            return 0

        lax.fori_loop(0, total_rows // 64, add, 0)
        last = links.copy(sent, far, {HEAD: over})
        last.start()
        for copy in copies:
            copy.wait_send()
        return last

    for k in range(head_count):
        r.branch[k] = product(
            r.hidden[...], r.v_w_out[:, k * piece : (k + 1) * piece]
        ).astype(LOW)
    branch_copies = spread_parts(r.branch, r.branch_near)
    if not paired:
        for k in range(head_count):
            columns = slice(k * piece, (k + 1) * piece)
            r.part_out[:, columns] = product(r.hidden[...], r.cot_all[k], 0, 0).astype(LOW)
        out_streams = [stream_start(bufs_out, c) for c in range(r.up_out.shape[0])]

    r.pair_weight[...] = jnp.zeros((seqs, rows, rows), WIDE)
    r.row_part[...] = jnp.zeros((seqs, rows, state), WIDE)
    r.col_part[...] = jnp.zeros((seqs, state, rows), WIDE)
    head_lane = iota((1, state), 1)

    upper_tri = iota((rows, rows), 0) <= iota((rows, rows), 1)

    def backward_pair(i, _):
        q, j = i // (heads // 2), lax.rem(i, heads // 2)
        at = block(j * state, state)
        grads, values = r.d_mixed_low[q, :, at], r.weighted[q, :, at]
        gram = r.gram[q]
        zero = jnp.zeros_like(grads)
        total = jnp.zeros((rows, state), WIDE)
        for part in range(2):
            g = 2 * j + part
            column = r.running_x[q, :, block(g * state, state)]
            gap = r.running_t[q, pl.ds(spare + g, 1), :] - jnp.concatenate(
                [column] * (rows // state), axis=1
            )
            decay = jnp.exp(jnp.where(upper_tri, gap, NEVER))
            kept = jnp.where(half_lane if part == 0 else ~half_lane, grads, zero)
            total = total + product((gram * decay).astype(LOW), kept)
            pairs = decay * product(values, kept, 1, 1)
            r.pair_weight[q] += pairs
            flows = pairs * gram
            r.row_part[q] += jnp.where(
                head_lane == spare + g, jnp.sum(flows, axis=1, keepdims=True), 0.0
            )
            r.col_part[q, pl.ds(spare + g, 1), :] = jnp.sum(flows, axis=0, keepdims=True)
        r.projected[q, :, at] = total
        return 0

    for q in range(seqs):
        r.gram[q] = product(r.b_all[q], r.c_all[q], 1, 1)
    backward_first = links.reserve(chunk_total)

    def backward_slot(i, _):
        backward_pair(i, 0)
        c = i - 2 * (seq_count - 1 - s)

        @pl.when((c >= 0) & (c < chunk_total))
        def _():
            hop(r.adj_in, r.state_local, r.adj_out, backward_first, c, False)

        return 0

    slots = chunk_total + 2 * (seq_count - 1)
    assert slots <= pair_total, slots
    lax.fori_loop(0, chunk_total, backward_slot, 0)
    branch_last = spread_over(r.branch, r.branch_near, r.sent, r.branch_far, branch_copies)
    if paired:
        send_normed.wait()
        send_cot.wait()

        @pl.when(s == 0)
        def _():
            out_grad()

    lax.fori_loop(chunk_total, pair_total, backward_slot, 0)

    for q in range(seqs):
        pairs = r.pair_weight[q].astype(LOW)
        d_in = product(pairs, r.c_all[q]) + product(r.weighted_tail[q], r.adj_in[q])
        d_out = product(pairs, r.b_all[q], 0, 0) + product(r.d_growth[q], r.state_in[q])
        r.sel_keep[q] = jnp.where(upper, d_out, d_in)
        r.sel_send[q] = jnp.where(upper, d_in, d_out).astype(LOW)
    sel_over = links.copy(r.sel_send, r.sel_over, {HEAD: over})
    sel_over.start()

    for q in range(seqs):
        running = r.running[q]
        tail = picked(jnp.exp(running[rows - 1 : rows, :] - running), r.expand[...], count=2)
        r.mixed[q] = product(r.b_all[q], r.adj_in[q], 1, 1) * tail

    def value_back(i, _):
        q, base = i // (rows // tile), lax.rem(i, rows // tile) * tile
        at = block(base, tile)
        inter_back = r.mixed[q, at, :]
        projected = r.projected[q, at, :] + inter_back
        step_x = r.step_x[q, at, :]
        d_mixed = r.d_mixed_low[q, at, :].astype(WIDE)
        act = r.act[q, at, :].astype(WIDE)
        d_value = projected * step_x + r.skip_x[0:1, :] * d_mixed
        conv = convolve(r.value_ext, q, base, tile, r.conv_value, value_bias)
        logistic = sigmoid(conv)
        r.slope_v[q, at, :] = d_value * (logistic * (1.0 + conv * (1.0 - logistic)))
        r.projected[q, at, :] = act * projected
        r.mixed[q, at, :] = act * step_x * inter_back
        r.inter[q, at, :] = d_mixed * r.inter[q, at, :]
        return 0

    lax.fori_loop(0, total_rows // tile, value_back, 0)
    rim_back = []
    for q in range(seqs):
        rim_back.append(
            links.copy(
                r.slope_v.at[q, 0:RIM, :],
                r.slope_v.at[q, rows : rows + RIM, :],
                {SEQ: lax.rem(s + seq_count - 1, seq_count)},
            )
        )

    @pl.when(s > 0)
    def _():
        for copy in rim_back:
            copy.start()

    if paired:

        @pl.when(s > 0)
        def _():
            out_grad()

    sel_over.wait()
    r.sel_pair[...] = (r.sel_keep[...] + r.sel_over[...].astype(WIDE)).astype(LOW)
    sel_side = links.copy(r.sel_pair, r.sel_side, {HEAD: side})
    sel_side.start()


    sel_side.wait()
    for q in range(seqs):
        total = r.sel_pair[q].astype(WIDE) + r.sel_side[q].astype(WIDE)
        conv = convolve(r.select_ext, q, 0, rows, r.taps, r.taps[4:5, :])
        logistic = sigmoid(conv)
        r.slope_s[q, 0:rows, :] = jnp.where(
            mine, total * (logistic * (1.0 + conv * (1.0 - logistic))), 0.0
        )
    rim_back_s = []
    for q in range(seqs):
        rim_back_s.append(
            links.copy(
                r.slope_s.at[q, 0:RIM, :],
                r.slope_s.at[q, rows : rows + RIM, :],
                {SEQ: lax.rem(s + seq_count - 1, seq_count)},
            )
        )

    @pl.when(s > 0)
    def _():
        for copy in rim_back_s:
            copy.start()

    @pl.when(s < seq_count - 1)
    def _():
        for copy in rim_back:
            copy.wait_recv()

    def conv_back(i, carry):
        q, base = i // (rows // tile), lax.rem(i, rows // tile) * tile
        at = block(base, tile)
        slopes = r.slope_v[q, pl.ds(pl.multiple_of(base, 8), tile + RIM), :]
        wide = r.value_ext[q, pl.ds(pl.multiple_of(base, 8), tile + RIM), :]
        grad = r.conv_value[0:1, :] * slopes[3 : 3 + tile]
        for k in range(1, 4):
            grad = grad + r.conv_value[k : k + 1, :] * slopes[3 - k : 3 - k + tile]
        r.gate[block(i * tile, tile), :] = grad.astype(LOW)
        own = slopes[0:tile]
        fresh = []
        for k in range(4):
            term = own * wide[RIM - 3 + k : RIM - 3 + k + tile]
            total = carry[k]
            for t in range(tile // 8):
                total = total + term[t * 8 : t * 8 + 8]
            fresh.append(total)
        total = carry[4]
        for t in range(tile // 8):
            total = total + own[t * 8 : t * 8 + 8]
        return tuple(fresh) + (total,)

    totals = lax.fori_loop(0, total_rows // tile, conv_back, (blank,) * 5)
    for k in range(5):
        small[k : k + 1, 0:inner] = jnp.sum(totals[k], axis=0, keepdims=True)
    if paired:
        send_value = chunk_sends(r.gate, r.far_value)
        stream_b(out_streams[0])
        stream_b(out_streams[1])
        pair_grad(r.part_gate, r.gate_low, r.far_gate, send_gate, gate_streams)
    else:
        big_grad(r.part_value, r.normed, r.gate[...], piece)
        value_streams = [stream_start(bufs_value, c) for c in range(r.up_value.shape[0])]
        for me in out_streams + gate_streams:
            stream_a(me)
        stream_b(out_streams[0])
        stream_b(out_streams[1])
    stream_c(out_streams[0])
    stream_b(out_streams[2])
    stream_c(out_streams[1])

    for q in range(seqs):
        step = r.step[q]
        rate = -jnp.exp(r.taps[6:7, :])
        expand = r.expand[...]
        direct = picked(r.projected[q], expand, 1, 1, 2)
        later = picked(r.inter[q], expand, 1, 1, 2)
        earlier = picked(r.mixed[q], expand, 1, 1, 2)
        crossing = r.state_in[q].astype(WIDE) * r.adj_in[q].astype(WIDE)
        bound = picked(picked_by(jnp.ones((8, state), LOW), crossing, 1, 1), expand, 1, 1)[0:1, :]
        last = r.running[q, rows - 1 : rows, :]
        d_log = (
            picked_by(tri[...], later - r.row_part[q], 0, 0)
            + picked_by(tri[...], r.col_part[q], 0, 1)
            + (picked_by(tri[...], earlier) - earlier)
            + bound * jnp.exp(last)
        )
        used = (head_lane >= spare) & (head_lane < spare + heads)
        d_step = direct + d_log * rate
        d_raw = jnp.where(used, d_step * sigmoid(r.step_arg[q]), 0.0)
        r.step_grad[q] = d_raw
        lanes = slice(inner + state, inner + 2 * state)
        small[0:1, lanes] += jnp.sum(d_raw, axis=0, keepdims=True)
        small[1:2, lanes] += jnp.where(used, jnp.sum(d_log * step, axis=0, keepdims=True) * rate, 0.0)


    @pl.when(s < seq_count - 1)
    def _():
        for copy in rim_back_s:
            copy.wait_recv()

    for q in range(seqs):
        slopes = r.slope_s[q]
        wide = r.select_ext[q]
        at = slice(inner, inner + state)
        grad = r.taps[0:1, :] * slopes[3 : 3 + rows]
        for k in range(1, 4):
            grad = grad + r.taps[k : k + 1, :] * slopes[3 - k : 3 - k + rows]
        own = slopes[0:rows]
        for k in range(4):
            small[k : k + 1, at] += jnp.sum(
                own * wide[RIM - 3 + k : RIM - 3 + k + rows], axis=0, keepdims=True
            )
        small[4:5, at] += jnp.sum(own, axis=0, keepdims=True)
        r.select_low[pl.ds(q * rows, rows), :] = jnp.where(mine, grad, r.step_grad[q]).astype(LOW)
    if paired:
        send_select = links.copy(r.select_low, r.far_select, mate)
        send_select.start()
    else:
        big_grad(r.part_select, r.select_low, r.normed[...], state)
        select_streams = [stream_start(bufs_select, 0)]
    stream_b(gate_streams[0])

    if paired:
        pair_grad(r.part_value, r.gate, r.far_value, send_value, value_streams)
        for copy in send_hidden:
            copy.wait_send()
    else:
        for me in value_streams + select_streams:
            stream_a(me)
    stream_c(out_streams[2])
    stream_b(gate_streams[1])
    stream_c(gate_streams[0])

    branch_last.wait()

    def output_rows(i, _):
        at = block(i * 64, 64)
        total = (
            r.branch[h, at, :].astype(WIDE)
            + r.branch_near[0, at, :].astype(WIDE)
            + r.branch_far[at, :].astype(WIDE)
        )
        r.o_block[at, :] = (r.x_all[h, at, :].astype(WIDE) + total).astype(LOW)
        return 0

    lax.fori_loop(0, total_rows // 64, output_rows, 0)
    for k in range(head_count):
        columns = slice(k * piece, (k + 1) * piece)

        def d_normed_rows(q, _):
            at = block(q * rows, rows)
            total = product(r.gate_low[at, :], r.v_w_gate[columns, :], 1, 1)
            total = total + product(r.gate[at, :], r.v_w_value[columns, :], 1, 1)
            total = total + product(r.select_low[at, :], r.v_w_select[:, columns])
            mean = jnp.sum(
                total * r.x_all[k, at, :].astype(WIDE) * r.gain_all[k, 0:1, :],
                axis=1,
                keepdims=True,
            )
            r.branch[k, at, :] = total.astype(LOW)
            if k == 0:
                r.sums[at, :] = jnp.where(iota((rows, state), 1) == 0, mean, 0.0)
            else:
                r.sums[at, :] += jnp.where(iota((rows, state), 1) == 0, mean, 0.0)
            return 0

        lax.fori_loop(0, seqs, d_normed_rows, 0)
    normed_copies = spread_parts(r.branch, r.normed_near)
    mean_copies = row_sums(r.mean_own, r.mean_held)
    stream_b(gate_streams[2])
    stream_c(gate_streams[1])
    stream_b(value_streams[0])
    normed_last = spread_over(r.branch, r.normed_near, r.sent, r.normed_far, normed_copies)
    row_sums_end(r.mean_own, r.mean_held, mean_copies)
    stream_c(gate_streams[2])
    stream_b(value_streams[1])
    normed_last.wait()

    def input_rows(i, total):
        at = block(i * 32, 32)
        grad = (
            r.branch[h, at, :].astype(WIDE)
            + r.normed_near[0, at, :].astype(WIDE)
            + r.normed_far[at, :].astype(WIDE)
        )
        own = r.x_all[h, at, :].astype(WIDE)
        inverse = r.inverse[at, 0:1]
        mean = r.sums[at, 0:1] / model
        r.o_input[at, :] = (
            r.cot_all[h, at, :].astype(WIDE)
            + inverse * (grad * r.gain_all[h, 0:1, :])
            - own * (inverse * inverse * inverse * mean)
        )
        term = grad * own * inverse
        for t in range(4):
            total = total + term[t * 8 : t * 8 + 8]
        return total

    gain_grad = lax.fori_loop(0, total_rows // 32, input_rows, jnp.zeros((8, piece), WIDE))
    small[7:8, 0:piece] = jnp.sum(gain_grad, axis=0, keepdims=True)

    if paired:
        send_select.wait()
        total = product(r.select_low[...], r.normed[:, own_half], 0, 0)
        total = total + product(r.far_select[...], r.far_normed[...], 0, 0)
        r.part_select[0] = total.astype(LOW)
        stream_up(select_streams[0])

    small_copies = []
    for j in range(1, seq_count):
        copy = links.copy(small, r.small_seq.at[j - 1], {SEQ: lax.rem(s + j, seq_count)})
        copy.start()
        small_copies.append(copy)
    stream_c(value_streams[0])
    stream_b(value_streams[2])
    stream_c(value_streams[1])
    stream_b(select_streams[0])
    stream_c(value_streams[2])
    total = small[...]
    for j, copy in enumerate(small_copies):
        copy.wait()
    for j in range(seq_count - 1):
        total = total + r.small_seq[j]
    r.small_mid[...] = total
    small_copies = []
    for j in range(1, dp_count):
        copy = links.copy(r.small_mid, r.small_dp.at[j - 1], {DP: lax.rem(d + j, dp_count)})
        copy.start()
        small_copies.append(copy)
    stream_c(select_streams[0])
    for copy in small_copies:
        copy.wait()
    for j in range(dp_count - 1):
        total = total + r.small_dp[j]
    r.o_small[:, 0:inner] = total[:, 0:inner]
    taps_grad, by_head = total[:, inner : inner + state], total[:, inner + state :]
    r.o_small[:, inner : inner + state] = jnp.where(odd, pltpu.roll(taps_grad, half, 1), taps_grad)
    r.o_small[:, inner + state :] = jnp.where(odd, by_head, pltpu.roll(by_head, half, 1))
    for me in keeps:
        stream_d(me)

    @pl.when(s > 0)
    def _():
        for copy in rim_back + rim_back_s:
            copy.wait_send()
        for c in range(chunk_total):
            hop_copy(r.adj_in, r.adj_out, backward_first, c, False)[1].wait_send()

    assert links.count <= size.links, links.count


def finish_kernel(half, heads, piece, inner, *refs):
    ins, outs = refs[:7], refs[7:]
    for source, target in zip(ins[:5], outs[:5]):
        target[...] = source[...].astype(target.dtype)
    matrix, small = ins[5:]
    g_select, g_step, g_norm, g_conv, g_bias, g_conv_s, g_bias_s, g_bias_h, g_decay, g_skip, g_gain = outs[5:]

    @pl.when(pl.program_id(0) == 0)
    def _():
        odd = lax.rem(lax.axis_index(HEAD), 2) == 1
        low_rows, high_rows = matrix[0:half, :].astype(WIDE), matrix[half : 2 * half, :].astype(WIDE)
        g_select[...] = jnp.where(odd, high_rows, low_rows)
        g_step[...] = jnp.where(odd, low_rows, high_rows)[0:heads, :]
        g_norm[...] = small[7, 0:piece]
        g_conv[...] = small[0:4, 0:inner]
        g_bias[...] = small[4, 0:inner]
        g_gain[...] = small[5, 0:inner]
        g_conv_s[...] = small[0:4, inner : inner + half]
        g_bias_s[...] = small[4, inner : inner + half]
        for row, target in enumerate((g_bias_h, g_decay, g_skip)):
            target[...] = small[row, inner + 2 * half : inner + 2 * half + heads]


def body(size, *args):
    (
        block_input,
        norm_gain,
        w_gate,
        w_value,
        w_select,
        w_step,
        conv_value,
        bias_value,
        conv_select,
        bias_select,
        step_bias,
        decay_log,
        skip_gain,
        gate_gain,
        w_out,
        out_cotangent,
    ) = args
    seqs, rows, piece = block_input.shape
    heads, inner = skip_gain.shape[0], w_value.shape[1]
    head_axis, seq_axis, dp_axis = size[HEAD], size[SEQ], size[DP]
    half = w_select.shape[1]
    state = half * head_axis // 2
    width = inner // heads
    model = piece * head_axis
    total_rows = seqs * rows
    assert head_axis == 4 and seq_axis == 4 and 2 * half == state and heads <= half and 2 * width == state

    vmem = pl.BlockSpec(memory_space=pltpu.VMEM)
    anywhere = pl.BlockSpec(memory_space=pl.ANY)
    inputs = dict(
        x=(block_input.reshape(total_rows, piece), anywhere),
        cot=(out_cotangent.reshape(total_rows, piece), anywhere),
        bias_value=(bias_value, vmem),
        gate_gain=(gate_gain, vmem),
        norm_gain=(norm_gain, vmem),
        bias_select=(bias_select, vmem),
        step_bias=(step_bias, vmem),
        decay_log=(decay_log, vmem),
        skip_gain=(skip_gain, vmem),
        conv_value=(conv_value, vmem),
        conv_select=(conv_select, vmem),
        w_select=(w_select.T, vmem),
        w_step=(w_step.T, vmem),
        w_value=(w_value, anywhere),
        w_gate=(w_gate, anywhere),
        w_out=(w_out, anywhere),
    )
    small_shape = (8, inner + 2 * state)

    def result(shape, kind, spec):
        return (jax.ShapeDtypeStruct(shape, kind), spec)

    outputs = dict(
        o_block=result((total_rows, piece), LOW, vmem),
        o_input=result((total_rows, piece), WIDE, vmem),
        o_small=result(small_shape, WIDE, vmem),
        out_out=result((inner, model), LOW, anywhere),
        out_gate=result((model, inner), LOW, anywhere),
        out_value=result((model, inner), LOW, anywhere),
        out_select=result((state, model), LOW, anywhere),
    )
    link_total = 128 + 16 * dp_axis

    def wide(*shape):
        return pltpu.VMEM(shape, WIDE)

    def low(*shape):
        return pltpu.VMEM(shape, LOW)

    def wide_tokens(lanes, extra=0):
        return wide(seqs, rows + extra, lanes)

    def low_tokens(lanes):
        return low(seqs, rows, lanes)

    def over_of(chunks, depth, columns):
        return low(chunks, dp_axis - 1, depth // (chunks * dp_axis), columns)

    def cut_of(chunks, depth, columns):
        return low(chunks, depth // (chunks * dp_axis), columns)

    semaphores = pltpu.SemaphoreType.DMA
    scratch = dict(
        send_sem=semaphores((link_total,)),
        recv_sem=semaphores((link_total,)),
        load_sem=semaphores((5,)),
        keep_sem=semaphores((10,)),
        v_w_select=low(state, model),
        v_w_value=low(model, inner),
        v_w_gate=low(model, inner),
        v_w_out=low(inner, model),
        gain_all=wide(head_axis, 8, piece),
        x_all=low(head_axis, total_rows, piece),
        cot_all=low(head_axis, total_rows, piece),
        normed=low(total_rows, model),
        inverse=wide(total_rows, state),
        expand=low(state, inner),
        tri=low(rows, rows),
        taps=wide(8, state),
        step_arg=wide_tokens(state),
        step=wide_tokens(state),
        running=wide_tokens(state),
        row_part=wide_tokens(state),
        step_grad=wide_tokens(state),
        sel_keep=wide_tokens(state),
        running_t=wide(seqs, state, rows),
        col_part=wide(seqs, state, rows),
        running_x=wide_tokens(heads * state),
        step_x=wide_tokens(inner),
        scale_x=wide_tokens(inner),
        mixed=wide_tokens(inner),
        inter=wide_tokens(inner),
        projected=wide_tokens(inner),
        act=low_tokens(inner),
        weighted=low_tokens(inner),
        weighted_tail=low_tokens(inner),
        d_mixed_low=low_tokens(inner),
        d_growth=low_tokens(inner),
        value_ext=wide_tokens(inner, RIM),
        select_ext=wide_tokens(state, RIM),
        slope_v=wide_tokens(inner, RIM),
        slope_s=wide_tokens(state, RIM),
        select_own=low_tokens(state),
        select_side=low_tokens(state),
        select_pair=low_tokens(state),
        select_over=low_tokens(state),
        b_all=low_tokens(state),
        c_all=low_tokens(state),
        sel_send=low_tokens(state),
        sel_over=low_tokens(state),
        sel_pair=low_tokens(state),
        sel_side=low_tokens(state),
        gram=wide(seqs, rows, rows),
        pair_weight=wide(seqs, rows, rows),
        state_local=wide(seqs, inner, state),
        decay_row=wide(seqs, inner, state),
        state_in=low(seqs, inner, state),
        state_out=low(seqs, inner, state),
        adj_in=low(seqs, inner, state),
        adj_out=low(seqs, inner, state),
        gate=low(total_rows, inner),
        hidden=low(total_rows, inner),
        gate_low=low(total_rows, inner),
        select_low=low(total_rows, state),
        skip_x=wide(8, inner),
        sums=wide(total_rows, state),
        sum_own=wide(8, total_rows),
        sum_held=wide(head_axis - 1, 8, total_rows),
        mean_own=wide(8, total_rows),
        mean_held=wide(head_axis - 1, 8, total_rows),
        branch=low(head_axis, total_rows, piece),
        sent=low(total_rows, piece),
        branch_near=low(2, total_rows, piece),
        branch_far=low(total_rows, piece),
        normed_near=low(2, total_rows, piece),
        normed_far=low(total_rows, piece),
        small=wide(*small_shape),
        small_mid=wide(*small_shape),
        small_seq=wide(seq_axis - 1, *small_shape),
        small_dp=wide(dp_axis - 1, *small_shape),
    )
    if dp_axis == 2:
        scratch.update(
            far_normed=low(total_rows, model // 2),
            far_cot=low(head_axis // 2, total_rows, piece),
            far_hidden=low(3, total_rows, inner // 3),
            far_gate=low(3, total_rows, inner // 3),
            far_value=low(3, total_rows, inner // 3),
            far_select=low(total_rows, state),
            part_out=low(3, inner // 3, model // 2),
            part_gate=low(3, model // 2, inner // 3),
            part_value=low(3, model // 2, inner // 3),
            part_select=low(1, state, model // 2),
            up_out=low(3, inner // 3, model // 2),
            mid_out=low(3, inner // 3, model // 2),
            up_gate=low(3, model // 2, inner // 3),
            mid_gate=low(3, model // 2, inner // 3),
            up_value=low(3, model // 2, inner // 3),
            mid_value=low(3, model // 2, inner // 3),
            up_select=low(1, state, model // 2),
            mid_select=low(1, state, model // 2),
        )
    else:
        scratch.update(
            part_out=low(inner, model),
            part_gate=low(model, inner),
            part_value=low(model, inner),
            part_select=low(state, model),
            over_out=over_of(3, inner, model),
            over_gate=over_of(3, model, inner),
            over_value=over_of(3, model, inner),
            over_select=over_of(1, state, model),
            up_out=cut_of(3, inner, model),
            up_gate=cut_of(3, model, inner),
            up_value=cut_of(3, model, inner),
            up_select=cut_of(1, state, model),
            mid_out=cut_of(3, inner, model),
            mid_gate=cut_of(3, model, inner),
            mid_value=cut_of(3, model, inner),
            mid_select=cut_of(1, state, model),
        )
    facts = SimpleNamespace(
        names=list(inputs) + list(outputs) + list(scratch),
        seqs=seqs,
        rows=rows,
        heads=heads,
        width=width,
        inner=inner,
        state=state,
        piece=piece,
        head_axis=head_axis,
        seq_axis=seq_axis,
        dp_axis=dp_axis,
        links=link_total,
    )
    results = pl.pallas_call(
        functools.partial(mixer_kernel, facts),
        out_shape=[shape for shape, _ in outputs.values()],
        in_specs=[spec for _, spec in inputs.values()],
        out_specs=[spec for _, spec in outputs.values()],
        scratch_shapes=list(scratch.values()),
        compiler_params=pltpu.CompilerParams(
            collective_id=0, has_side_effects=True, vmem_limit_bytes=67043328
        ),
    )(*[value for value, _ in inputs.values()])
    got = SimpleNamespace(**dict(zip(outputs, results, strict=True)))
    steps = 4

    def by_rows(depth, columns):
        return pl.BlockSpec((depth // steps, columns), lambda i: (i, 0))

    def whole(*shape):
        return pl.BlockSpec(shape, lambda i: (0,) * len(shape))

    streamed = [(total_rows, piece), (total_rows, piece), (inner, model), (model, inner), (model, inner)]
    kinds = [LOW, WIDE, WIDE, WIDE, WIDE]
    fixed = [
        (half, model),
        (heads, model),
        (piece,),
        (4, inner),
        (inner,),
        (4, half),
        (half,),
        (heads,),
        (heads,),
        (heads,),
        (inner,),
    ]
    final = pl.pallas_call(
        functools.partial(finish_kernel, half, heads, piece, inner),
        grid=(steps,),
        out_shape=[jax.ShapeDtypeStruct(shape, kind) for shape, kind in zip(streamed, kinds)]
        + [jax.ShapeDtypeStruct(shape, WIDE) for shape in fixed],
        in_specs=[by_rows(*shape) for shape in streamed]
        + [whole(state, model), whole(*small_shape)],
        out_specs=[by_rows(*shape) for shape in streamed] + [whole(*shape) for shape in fixed],
    )(
        got.o_block,
        got.o_input,
        got.out_out,
        got.out_gate,
        got.out_value,
        got.out_select,
        got.o_small,
    )
    block_output, input_grad, g_out, g_gate, g_value, g_select, g_step = final[:7]
    g_norm, g_conv, g_bias, g_conv_s, g_bias_s, g_step_bias, g_decay, g_skip, g_gain = final[7:]
    return (
        block_output.reshape(seqs, rows, piece),
        input_grad.reshape(seqs, rows, piece),
        g_norm,
        g_gate,
        g_value,
        g_select.T,
        g_step.T,
        g_conv,
        g_bias,
        g_conv_s,
        g_bias_s,
        g_step_bias,
        g_decay,
        g_skip,
        g_gain,
        g_out,
    )


def solution(mesh):
    columns, single, tokens = P(None, HEAD), P(HEAD), P(DP, SEQ, HEAD)
    in_specs = (
        tokens,
        single,
        columns,
        columns,
        columns,
        columns,
        columns,
        single,
        columns,
        single,
        single,
        single,
        single,
        single,
        P(HEAD, None),
        tokens,
    )
    out_specs = (
        tokens,
        tokens,
        single,
        columns,
        columns,
        columns,
        columns,
        columns,
        single,
        columns,
        single,
        single,
        single,
        single,
        single,
        P(HEAD, None),
    )
    return jax.shard_map(
        functools.partial(body, dict(mesh.shape)),
        mesh=mesh,
        in_specs=in_specs,
        out_specs=out_specs,
        check_vma=False,
    )
```
